32 devices in a mesh: batch: 8 (over z, x), chan: 4 (over y, core).
Axes of the slice: x: 2, y: 2, z: 4, core: 2. Of those that a mesh axis runs over, the one named last changes fastest.
Arguments:
- signal: float32 [1024, 32768], P('chan', 'batch'), may hold values from -6 to 6
- cotangent: float32 [1024, 32768], P('chan', 'batch'), may hold values from -6 to 6
- first_layer: float32 [33, 64], replicated, may hold values from -5 to 5
- second_layer: float32 [64, 1024], P(None, 'chan'), may hold values from -0.75 to 0.75
- decay_rate: float32 [1024], P('chan'), may hold values from 0.3 to 600
- skip_gain: float32 [1024], P('chan'), may hold values from -4 to 4
Outputs:
- input_grad: float32 [1024, 32768], P('chan', 'batch')
- first_grad: float32 [33, 64], replicated
- second_grad: float32 [64, 1024], P(None, 'chan')
- decay_grad: float32 [1024], P('chan')
- skip_grad: float32 [1024], P('chan')
The draws below stay inside these ranges and needn't reach their ends.
All inputs are finite; a program needn't handle non-finite values.
Results may differ from the reference program's by a relative error of at most 0.0003.
Values sent between devices are 32-bit elements; how exact they have to be, the bound alone decides.
A program may use at most 256 MiB of HBM per device.

```python
import math
import jax
import jax.numpy as jnp
from jax import lax

WIDTH = 1024
LENGTH = 32768
ORDER = 64
BANDS = 16
EMBED = 33


def block_levels(key, shape, pieces, smallest, top_value):
    gain, own = 1.0, jax.random.fold_in(key, 6)
    for position, parts in pieces:
        heights = jnp.exp(jax.random.uniform(jax.random.fold_in(own, position), (parts,), jnp.float32, smallest / len(pieces), top_value / len(pieces)))
        gain = gain * jnp.repeat(heights, shape[position] // parts).reshape([-1 if axis == position else 1 for axis in range(len(shape))])
    return gain


def scatter_about(own_key, extent, deviation, reach, split=(), kind=jnp.bfloat16):
    result = deviation * jax.random.normal(own_key, extent, jnp.float32)
    if split:
        result = result * block_levels(own_key, extent, split, -0.22, 0.18)
    return jnp.clip(result, -reach, reach).astype(kind)


def setup_inputs(seed: int = 0) -> dict:
    key_of = jax.random.split(jax.random.key(seed), 7)
    return {
        "signal": scatter_about(key_of[0], (WIDTH, LENGTH), 1.0, 6.0, ((0, 4), (1, 8)), jnp.float32),
        "cotangent": scatter_about(key_of[1], (WIDTH, LENGTH), 1.0, 6.0, ((0, 4), (1, 8)), jnp.float32),
        "first_layer": scatter_about(key_of[2], (EMBED, ORDER), 1.0, 5.0, (), jnp.float32),
        "second_layer": scatter_about(key_of[3], (ORDER, WIDTH), ORDER ** -0.5, 0.75, ((1, 4),), jnp.float32),
        "decay_rate": jnp.clip(jnp.exp(math.log(600.0) - 7.6009024 * jax.random.uniform(key_of[4], (WIDTH,), jnp.float32) ** block_levels(key_of[4], (WIDTH,), ((0, 4),), -0.2, 0.2)), 0.3, 600.0),
        "skip_gain": scatter_about(key_of[5], (WIDTH,), 1.0, 4.0, ((0, 4),), jnp.float32),
    }


precise = lax.Precision.HIGHEST
epsilon = 1e-06

def features(positions, length, band_count):
    band_index = jnp.arange(1, band_count + 1, dtype=jnp.int32)
    phase = (band_index[:, None] * positions[None, :] % length).astype(jnp.float32) * (2.0 * math.pi / length)
    linear = positions.astype(jnp.float32)[None, :] / length
    return jnp.concatenate([linear, jnp.cos(phase), jnp.sin(phase)], axis=0)

def reference(signal, cotangent, first_layer, second_layer, decay_rate, skip_gain):
    positions = jnp.arange(LENGTH, dtype=jnp.int32)
    embed = features(positions, LENGTH, BANDS)
    before = jnp.dot(first_layer.T, embed, precision=precise)
    basis = jnp.sin(before)
    fraction = positions.astype(jnp.float32) / LENGTH
    factor = 1.0 / math.sqrt(LENGTH)
    padded = 2 * LENGTH
    stride = 64
    blocks_count = WIDTH // stride

    def step(carry, index):
        start = (index * stride).astype(jnp.int32)
        values = lax.dynamic_slice_in_dim(signal, start, stride, 0)
        cotan = lax.dynamic_slice_in_dim(cotangent, start, stride, 0)
        columns = lax.dynamic_slice_in_dim(second_layer, start, stride, 1)
        rates = lax.dynamic_slice_in_dim(decay_rate, start, stride, 0)
        gains = lax.dynamic_slice_in_dim(skip_gain, start, stride, 0)
        window = jnp.exp(-rates[:, None] * fraction[None, :])
        shaped = window * jnp.dot(columns.T, basis, precision=precise)
        norms = jnp.sqrt(lax.optimization_barrier(jnp.sum(shaped * shaped, axis=1, keepdims=True)) + epsilon)
        filt = shaped / norms
        spec_val = jnp.fft.rfft(values, n=padded)
        spec_cot = jnp.fft.rfft(cotan, n=padded)
        spec_filt = jnp.fft.rfft(filt, n=padded)
        in_grad = jnp.fft.irfft(jnp.conj(spec_filt) * spec_cot, n=padded)[:, :LENGTH] + gains[:, None] * cotan
        dfilt = factor * jnp.fft.irfft(jnp.conj(spec_val) * spec_cot, n=padded)[:, :LENGTH]
        skip_part = factor * lax.optimization_barrier(jnp.sum(cotan * values, axis=1))
        project = lax.optimization_barrier(jnp.sum(filt * dfilt, axis=1, keepdims=True))
        draw = (dfilt - filt * project) / norms
        decay_part = -lax.optimization_barrier(jnp.sum(draw * shaped * fraction[None, :], axis=1))
        dmix = draw * window
        second_part = jnp.dot(basis, dmix.T, precision=precise)
        carry = carry + jnp.dot(columns, dmix, precision=precise)
        return (carry, (in_grad.astype(jnp.float32), second_part, decay_part, skip_part))
    dbasis, results = lax.scan(step, jnp.zeros((ORDER, LENGTH), jnp.float32), jnp.arange(blocks_count, dtype=jnp.int32))
    in_blocks, second_blocks, decay_blocks, skip_blocks = results
    input_grad = in_blocks.reshape(WIDTH, LENGTH)
    second_grad = jnp.transpose(second_blocks, (1, 0, 2)).reshape(ORDER, WIDTH)
    decay_grad = decay_blocks.reshape(WIDTH)
    skip_grad = skip_blocks.reshape(WIDTH)
    first_grad = jnp.dot(embed, (jnp.cos(before) * dbasis).T, precision=precise)
    return (input_grad, first_grad, second_grad, decay_grad, skip_grad)
```

```python
import functools
import math

import jax
import jax.numpy as jnp
import numpy as np
from jax import lax
from jax.experimental import pallas as pl
from jax.experimental.pallas import tpu as pltpu
from jax.sharding import PartitionSpec as P

LANES = 128

exact = lax.Precision.HIGHEST
precise = lax.Precision.HIGH
epsilon = 1e-06


def sincos(x):
    turns = jnp.round(x * (2.0 / math.pi))
    r = x - turns * 1.5703125
    r = r - turns * 4.837512969970703125e-4
    r = r - turns * 7.549789948768648e-8
    sq = r * r
    sine = r + r * sq * (-1.6666654611e-1 + sq * (8.3321608736e-3 + sq * -1.9515295891e-4))
    cosine = 1.0 - 0.5 * sq + sq * sq * (
        4.166664568298827e-2 + sq * (-1.388731625493765e-3 + sq * 2.443315711809948e-5)
    )
    quadrant = turns.astype(jnp.int32) & 3
    odd = (quadrant & 1) == 1
    sin_value = jnp.where(odd, cosine, sine)
    cos_value = jnp.where(odd, sine, cosine)
    sin_value = jnp.where(quadrant >= 2, -sin_value, sin_value)
    cos_value = jnp.where((quadrant == 1) | (quadrant == 2), -cos_value, cos_value)
    return sin_value, cos_value


def features(positions, length, band_count):
    band_index = jnp.arange(1, band_count + 1, dtype=jnp.int32)
    phase = (band_index[:, None] * positions[None, :] % length).astype(jnp.float32) * (
        2.0 * math.pi / length
    )
    linear = positions.astype(jnp.float32)[None, :] / length
    sines, cosines = sincos(phase)
    return jnp.concatenate([linear, cosines, sines], axis=0)


def pair(matrix):
    high = matrix.astype(np.float32).astype(jnp.bfloat16)
    low = (matrix - high.astype(np.float64)).astype(np.float32).astype(jnp.bfloat16)
    return jnp.asarray(high), jnp.asarray(low)


def tables(rows, cols):
    r = np.arange(rows, dtype=np.float64)
    c = np.arange(cols, dtype=np.float64)
    first = 2.0 * np.pi * np.outer(r + 0.5, r) / (2 * rows)
    twist = 2.0 * np.pi * np.outer(r + 0.5, c) / (2 * rows * cols)
    angle = 2.0 * np.pi * (np.outer(c, c) % cols) / cols
    cos_c, sin_c = np.cos(angle), np.sin(angle)
    stage1 = np.concatenate([np.cos(first), -np.sin(first)], axis=0)
    stage2 = np.block([[cos_c, -sin_c], [sin_c, cos_c]])
    last = np.concatenate([np.cos(first.T), -np.sin(first.T)], axis=1) / (rows * cols)
    return (
        *pair(stage1),
        *pair(stage2),
        *pair(stage2.T.copy()),
        *pair(last),
        jnp.asarray(np.cos(twist), jnp.float32),
        jnp.asarray(np.sin(twist), jnp.float32),
    )


def split(x):
    high = x.astype(jnp.bfloat16)
    return high, (x - high.astype(jnp.float32)).astype(jnp.bfloat16)


def dot(a, b):
    return jnp.dot(a, b, preferred_element_type=jnp.float32)


def product(left, right):
    return dot(left[0], right[0]) + (dot(left[1], right[0]) + dot(left[0], right[1]))


def forward(arrays, first, second, cos_t, sin_t):
    rows, cols = cos_t.shape
    t = product(first, split(jnp.concatenate(arrays, axis=1)))
    parts = []
    for i in range(len(arrays)):
        re = t[:rows, i * cols : (i + 1) * cols]
        im = t[rows:, i * cols : (i + 1) * cols]
        parts.append(jnp.concatenate([re * cos_t + im * sin_t, im * cos_t - re * sin_t], axis=1))
    spec = product(split(jnp.concatenate(parts, axis=0)), second)
    return [
        (spec[i * rows : (i + 1) * rows, :cols], spec[i * rows : (i + 1) * rows, cols:])
        for i in range(len(arrays))
    ]


def backward(spectra, third, last, cos_t, sin_t):
    rows, cols = cos_t.shape
    prods = jnp.concatenate([jnp.concatenate(s, axis=1) for s in spectra], axis=0)
    back = product(split(prods), third)
    turns = []
    for i in range(len(spectra)):
        re, im = back[i * rows : (i + 1) * rows, :cols], back[i * rows : (i + 1) * rows, cols:]
        turns.append(
            jnp.concatenate([re * cos_t - im * sin_t, im * cos_t + re * sin_t], axis=0)
        )
    out = product(last, split(jnp.concatenate(turns, axis=1)))
    return [out[:, i * cols : (i + 1) * cols] for i in range(len(spectra))]


def read(ref, lane, group):
    if len(ref.shape) == 3:
        return ref[0, pl.ds(lane, ref.shape[1] // group, stride=group), :]
    count = ref.shape[2] // group
    return jnp.concatenate(
        [ref[b, 0, pl.ds(lane, count, stride=group), :] for b in range(ref.shape[0])], axis=0
    )


def write(ref, lane, group, value):
    if len(ref.shape) == 3:
        ref[0, pl.ds(lane, ref.shape[1] // group, stride=group), :] = value
        return
    count = ref.shape[2] // group
    for b in range(ref.shape[0]):
        ref[b, 0, pl.ds(lane, count, stride=group), :] = value[b * count : (b + 1) * count]


def kernel(group, a, b, w1h, w1l, w2h, w2l, w3h, w3l, w4h, w4l, ct, st, out):
    cos_t, sin_t = ct[...], st[...]
    first, second = (w1h[...], w1l[...]), (w2h[...], w2l[...])
    third, last = (w3h[...], w3l[...]), (w4h[...], w4l[...])
    count = 2 if group % 2 == 0 else 1

    def step(i, carry):
        lanes = [i * count + j for j in range(count)]
        xs = [read(a, lane, group) for lane in lanes] + [read(b, lane, group) for lane in lanes]
        specs = forward(xs, first, second, cos_t, sin_t)
        prods = []
        for (a_re, a_im), (b_re, b_im) in zip(specs[:count], specs[count:]):
            prods.append((a_re * b_re + a_im * b_im, a_re * b_im - a_im * b_re))
        for lane, value in zip(lanes, backward(prods, third, last, cos_t, sin_t)):
            write(out, lane, group, value)
        return carry

    lax.fori_loop(0, group // count, step, 0)


def correlate(a, b, out_shape, group, name, tabs):
    groups = b.shape[1]

    def spec(shape):
        if len(shape) == 3:
            return pl.BlockSpec((1, *shape[1:]), lambda i: (i, 0, 0))
        return pl.BlockSpec((shape[0], 1, *shape[2:]), lambda i: (0, i, 0, 0))

    rows, cols = tabs[-1].shape
    flops = 2 * 3 * groups * group * rows * cols * 3 * (2 * rows + 4 * cols)
    return pl.pallas_call(
        functools.partial(kernel, group),
        grid=(groups,),
        in_specs=[spec(a.shape), spec(b.shape)]
        + [pl.BlockSpec(t.shape, lambda i: (0, 0)) for t in tabs],
        out_specs=spec(out_shape),
        out_shape=jax.ShapeDtypeStruct(out_shape, jnp.float32),
        compiler_params=pltpu.CompilerParams(vmem_limit_bytes=56 * 1024 * 1024),
        cost_estimate=pl.CostEstimate(
            flops=flops, bytes_accessed=3 * 4 * a.size, transcendentals=0
        ),
        name=name,
    )(a, b, *tabs)


def local(signal, cotangent, first_layer, second_layer, decay_rate, skip_gain):
    parts = lax.axis_size("batch")
    place = lax.axis_index("batch")
    width_dev, local_len = signal.shape
    length = local_len * parts
    factor = 1.0 / math.sqrt(length)
    narrow = width_dev // parts
    group = min(8, narrow)
    groups = narrow // group
    rows = length // LANES
    tabs = tables(rows, LANES)

    def spread(x):
        x = x.reshape(parts, groups, group, local_len // LANES, LANES)
        x = x.transpose(0, 1, 3, 2, 4).reshape(parts, groups, -1, LANES)
        return lax.all_to_all(x, "batch", split_axis=0, concat_axis=0, tiled=True)

    def tiled(x):
        x = x.reshape(groups, group, rows, LANES).transpose(0, 2, 1, 3)
        return x.reshape(groups, rows * group, LANES)

    cot = spread(cotangent)
    positions = jnp.arange(length, dtype=jnp.int32)
    columns = lax.dynamic_slice_in_dim(second_layer, place * narrow, narrow, 1)
    rates = lax.dynamic_slice_in_dim(decay_rate, place * narrow, narrow, 0)
    gains = lax.dynamic_slice_in_dim(skip_gain, place * narrow, narrow, 0)
    embed = features(positions, length, first_layer.shape[0] // 2)
    before = jnp.dot(first_layer.T, embed, precision=exact)
    basis, slope = sincos(before)
    fraction = positions.astype(jnp.float32) / length
    window = jnp.exp(-rates[:, None] * fraction[None, :])
    shaped = window * jnp.dot(columns.T, basis, precision=precise)
    norms = jnp.sqrt(jnp.sum(shaped * shaped, axis=1, keepdims=True) + epsilon)
    filt = shaped / norms
    taps = tiled(filt + jnp.where(positions[None, :] == 0, gains[:, None], 0.0))
    cot, signal, taps, basis, slope = lax.optimization_barrier((cot, signal, taps, basis, slope))
    val = spread(signal)
    in_grad = correlate(taps, cot, cot.shape, group, "input_grad", tabs)
    val, in_grad = lax.optimization_barrier((val, in_grad))
    input_grad = lax.all_to_all(in_grad, "batch", split_axis=0, concat_axis=0, tiled=True)
    filt_grad = correlate(val, cot, taps.shape, group, "filter_grad", tabs)
    input_grad = input_grad.reshape(parts, groups, local_len // LANES, group, LANES)
    input_grad = input_grad.transpose(0, 1, 3, 2, 4).reshape(width_dev, local_len)
    filt_grad = filt_grad.reshape(groups, rows, group, LANES).transpose(0, 2, 1, 3)
    dfilt = factor * filt_grad.reshape(narrow, length)
    skip_part = (cot * val).reshape(parts, groups, local_len // LANES, group, LANES)
    skip_part = factor * jnp.sum(skip_part, axis=(0, 2, 4)).reshape(narrow)
    project = jnp.sum(filt * dfilt, axis=1, keepdims=True)
    draw = (dfilt - filt * project) / norms
    decay_part = -jnp.sum(draw * shaped * fraction[None, :], axis=1)
    dmix = draw * window
    second_part = jnp.dot(basis, dmix.T, precision=precise)
    dbasis = jnp.dot(columns, dmix, precision=precise)
    first_part = jnp.dot(embed, (slope * dbasis).T, precision=precise)
    packed = jnp.concatenate([second_part, decay_part[None], skip_part[None]], axis=0)
    packed, first_part, input_grad = lax.optimization_barrier((packed, first_part, input_grad))
    packed = lax.all_gather(packed, "batch", axis=1, tiled=True)
    first_grad = lax.psum(first_part, ("batch", "chan"))
    order = second_layer.shape[0]
    return (input_grad, first_grad, packed[:order], packed[order], packed[order + 1])


def solution(mesh):
    placed = (P("chan", "batch"), P("chan", "batch"), P(), P(None, "chan"), P("chan"), P("chan"))
    return jax.shard_map(
        local,
        mesh=mesh,
        in_specs=placed,
        out_specs=(P("chan", "batch"), P(), P(None, "chan"), P("chan"), P("chan")),
        check_vma=False,
    )
```

```python
import functools
import math

import jax
import jax.numpy as jnp
import numpy as np
from jax import lax
from jax.experimental import pallas as pl
from jax.experimental.pallas import tpu as pltpu
from jax.sharding import PartitionSpec as P

LANES = 128

exact = lax.Precision.HIGHEST
precise = lax.Precision.HIGH
epsilon = 1e-06


def sincos(x):
    turns = jnp.round(x * (2.0 / math.pi))
    r = x - turns * 1.5703125
    r = r - turns * 4.837512969970703125e-4
    r = r - turns * 7.549789948768648e-8
    sq = r * r
    sine = r + r * sq * (-1.6666654611e-1 + sq * (8.3321608736e-3 + sq * -1.9515295891e-4))
    cosine = 1.0 - 0.5 * sq + sq * sq * (
        4.166664568298827e-2 + sq * (-1.388731625493765e-3 + sq * 2.443315711809948e-5)
    )
    quadrant = turns.astype(jnp.int32) & 3
    odd = (quadrant & 1) == 1
    sin_value = jnp.where(odd, cosine, sine)
    cos_value = jnp.where(odd, sine, cosine)
    sin_value = jnp.where(quadrant >= 2, -sin_value, sin_value)
    cos_value = jnp.where((quadrant == 1) | (quadrant == 2), -cos_value, cos_value)
    return sin_value, cos_value


def features(positions, length, band_count):
    band_index = jnp.arange(1, band_count + 1, dtype=jnp.int32)
    phase = (band_index[:, None] * positions[None, :] % length).astype(jnp.float32) * (
        2.0 * math.pi / length
    )
    linear = positions.astype(jnp.float32)[None, :] / length
    sines, cosines = sincos(phase)
    return jnp.concatenate([linear, cosines, sines], axis=0)


def pair(matrix):
    high = matrix.astype(np.float32).astype(jnp.bfloat16)
    low = (matrix - high.astype(np.float64)).astype(np.float32).astype(jnp.bfloat16)
    return jnp.asarray(high), jnp.asarray(low)


def tables(rows, cols):
    r = np.arange(rows, dtype=np.float64)
    c = np.arange(cols, dtype=np.float64)
    first = 2.0 * np.pi * np.outer(r + 0.5, r) / (2 * rows)
    twist = 2.0 * np.pi * np.outer(r + 0.5, c) / (2 * rows * cols)
    angle = 2.0 * np.pi * (np.outer(c, c) % cols) / cols
    cos_c, sin_c = np.cos(angle), np.sin(angle)
    stage1 = np.concatenate([np.cos(first), -np.sin(first)], axis=0)
    stage2 = np.block([[cos_c, -sin_c], [sin_c, cos_c]])
    last = np.concatenate([np.cos(first.T), -np.sin(first.T)], axis=1) / (rows * cols)
    return (
        *pair(stage1),
        *pair(stage2),
        *pair(stage2.T.copy()),
        *pair(last),
        jnp.asarray(np.cos(twist), jnp.float32),
        jnp.asarray(np.sin(twist), jnp.float32),
    )


def split(x):
    high = x.astype(jnp.bfloat16)
    return high, (x - high.astype(jnp.float32)).astype(jnp.bfloat16)


def dot(a, b):
    return jnp.dot(a, b, preferred_element_type=jnp.float32)


def product(left, right):
    return dot(left[0], right[0]) + (dot(left[1], right[0]) + dot(left[0], right[1]))


def forward(arrays, first, second, cos_t, sin_t):
    rows, cols = cos_t.shape
    t = product(first, split(jnp.concatenate(arrays, axis=1)))
    parts = []
    for i in range(len(arrays)):
        re = t[:rows, i * cols : (i + 1) * cols]
        im = t[rows:, i * cols : (i + 1) * cols]
        parts.append(jnp.concatenate([re * cos_t + im * sin_t, im * cos_t - re * sin_t], axis=1))
    spec = product(split(jnp.concatenate(parts, axis=0)), second)
    return [
        (spec[i * rows : (i + 1) * rows, :cols], spec[i * rows : (i + 1) * rows, cols:])
        for i in range(len(arrays))
    ]


def backward(spectra, third, last, cos_t, sin_t):
    rows, cols = cos_t.shape
    prods = jnp.concatenate([jnp.concatenate(s, axis=1) for s in spectra], axis=0)
    back = product(split(prods), third)
    turns = []
    for i in range(len(spectra)):
        re, im = back[i * rows : (i + 1) * rows, :cols], back[i * rows : (i + 1) * rows, cols:]
        turns.append(
            jnp.concatenate([re * cos_t - im * sin_t, im * cos_t + re * sin_t], axis=0)
        )
    out = product(last, split(jnp.concatenate(turns, axis=1)))
    return [out[:, i * cols : (i + 1) * cols] for i in range(len(spectra))]


def read(ref, lane, group):
    if len(ref.shape) == 3:
        return ref[0, pl.ds(lane, ref.shape[1] // group, stride=group), :]
    count = ref.shape[2] // group
    return jnp.concatenate(
        [ref[b, 0, pl.ds(lane, count, stride=group), :] for b in range(ref.shape[0])], axis=0
    )


def write(ref, lane, group, value):
    if len(ref.shape) == 3:
        ref[0, pl.ds(lane, ref.shape[1] // group, stride=group), :] = value
        return
    count = ref.shape[2] // group
    for b in range(ref.shape[0]):
        ref[b, 0, pl.ds(lane, count, stride=group), :] = value[b * count : (b + 1) * count]


def kernel(group, a, b, w1h, w1l, w2h, w2l, w3h, w3l, w4h, w4l, ct, st, out):
    cos_t, sin_t = ct[...], st[...]
    first, second = (w1h[...], w1l[...]), (w2h[...], w2l[...])
    third, last = (w3h[...], w3l[...]), (w4h[...], w4l[...])
    count = 2 if group % 2 == 0 else 1

    def step(i, carry):
        lanes = [i * count + j for j in range(count)]
        xs = [read(a, lane, group) for lane in lanes] + [read(b, lane, group) for lane in lanes]
        specs = forward(xs, first, second, cos_t, sin_t)
        prods = []
        for (a_re, a_im), (b_re, b_im) in zip(specs[:count], specs[count:]):
            prods.append((a_re * b_re + a_im * b_im, a_re * b_im - a_im * b_re))
        for lane, value in zip(lanes, backward(prods, third, last, cos_t, sin_t)):
            write(out, lane, group, value)
        return carry

    lax.fori_loop(0, group // count, step, 0)


def correlate(a, b, out_shape, group, name, tabs):
    groups = b.shape[1]

    def spec(shape):
        if len(shape) == 3:
            return pl.BlockSpec((1, *shape[1:]), lambda i: (i, 0, 0))
        return pl.BlockSpec((shape[0], 1, *shape[2:]), lambda i: (0, i, 0, 0))

    rows, cols = tabs[-1].shape
    flops = 2 * 3 * groups * group * rows * cols * 3 * (2 * rows + 4 * cols)
    return pl.pallas_call(
        functools.partial(kernel, group),
        grid=(groups,),
        in_specs=[spec(a.shape), spec(b.shape)]
        + [pl.BlockSpec(t.shape, lambda i: (0, 0)) for t in tabs],
        out_specs=spec(out_shape),
        out_shape=jax.ShapeDtypeStruct(out_shape, jnp.float32),
        compiler_params=pltpu.CompilerParams(vmem_limit_bytes=56 * 1024 * 1024),
        cost_estimate=pl.CostEstimate(
            flops=flops, bytes_accessed=3 * 4 * a.size, transcendentals=0
        ),
        name=name,
    )(a, b, *tabs)


MESH = pl.DeviceIdType.MESH


def share_kernel(parts, chans, mine, shared, total, slots, partial, sums, sends, arrivals, sends2, arrivals2):
    me, my_chan = lax.axis_index("batch"), lax.axis_index("chan")
    barrier = pltpu.get_barrier_semaphore()
    for k in range(1, parts):
        peer = lax.rem(me + k, parts)
        pl.semaphore_signal(barrier, inc=1, device_id=(peer, my_chan), device_id_type=MESH)
    for k in range(1, chans):
        peer = lax.rem(my_chan + k, chans)
        pl.semaphore_signal(barrier, inc=1, device_id=(me, peer), device_id_type=MESH)
    pl.semaphore_wait(barrier, parts + chans - 2)
    copies = []
    for k in range(1, parts):
        copies.append(
            pltpu.make_async_remote_copy(
                src_ref=mine,
                dst_ref=slots.at[k],
                send_sem=sends.at[k],
                recv_sem=arrivals.at[k],
                device_id=(lax.rem(me + k, parts), my_chan),
                device_id_type=MESH,
            )
        )
        copies[-1].start()
    slots[0] = mine[...]
    for copy in copies:
        copy.wait_recv()
    acc = jnp.zeros(mine.shape, jnp.float32)
    for b in range(parts):
        block = slots[lax.rem(me + parts - b, parts)]
        shared[b] = block
        acc = acc + block
    partial[...] = acc
    for copy in copies:
        copy.wait_send()
    copies = []
    for k in range(1, chans):
        copies.append(
            pltpu.make_async_remote_copy(
                src_ref=partial,
                dst_ref=sums.at[k],
                send_sem=sends2.at[k],
                recv_sem=arrivals2.at[k],
                device_id=(me, lax.rem(my_chan + k, chans)),
                device_id_type=MESH,
            )
        )
        copies[-1].start()
    sums[0] = acc
    for copy in copies:
        copy.wait_recv()
    acc = jnp.zeros_like(acc)
    for c in range(chans):
        acc = acc + sums[lax.rem(my_chan + chans - c, chans)]
    total[...] = acc
    for copy in copies:
        copy.wait_send()


def share(block, parts, chans):
    vmem = pl.BlockSpec(memory_space=pltpu.VMEM)
    dma = pltpu.SemaphoreType.DMA
    return pl.pallas_call(
        functools.partial(share_kernel, parts, chans),
        in_specs=[vmem],
        out_specs=[vmem, vmem],
        out_shape=[
            jax.ShapeDtypeStruct((parts, *block.shape), jnp.float32),
            jax.ShapeDtypeStruct(block.shape, jnp.float32),
        ],
        scratch_shapes=[
            pltpu.VMEM((parts, *block.shape), jnp.float32),
            pltpu.VMEM(block.shape, jnp.float32),
            pltpu.VMEM((chans, *block.shape), jnp.float32),
            dma((parts,)),
            dma((parts,)),
            dma((chans,)),
            dma((chans,)),
        ],
        compiler_params=pltpu.CompilerParams(collective_id=0, has_side_effects=True),
        name="share",
    )(block)


def local(signal, cotangent, first_layer, second_layer, decay_rate, skip_gain):
    parts = lax.axis_size("batch")
    place = lax.axis_index("batch")
    width_dev, local_len = signal.shape
    length = local_len * parts
    factor = 1.0 / math.sqrt(length)
    narrow = width_dev // parts
    group = min(8, narrow)
    groups = narrow // group
    rows = length // LANES
    tabs = tables(rows, LANES)

    def spread(x):
        x = x.reshape(parts, groups, group, local_len // LANES, LANES)
        x = x.transpose(0, 1, 3, 2, 4).reshape(parts, groups, -1, LANES)
        return lax.all_to_all(x, "batch", split_axis=0, concat_axis=0, tiled=True)

    def tiled(x):
        x = x.reshape(groups, group, rows, LANES).transpose(0, 2, 1, 3)
        return x.reshape(groups, rows * group, LANES)

    cot = spread(cotangent)
    positions = jnp.arange(length, dtype=jnp.int32)
    columns = lax.dynamic_slice_in_dim(second_layer, place * narrow, narrow, 1)
    rates = lax.dynamic_slice_in_dim(decay_rate, place * narrow, narrow, 0)
    gains = lax.dynamic_slice_in_dim(skip_gain, place * narrow, narrow, 0)
    embed = features(positions, length, first_layer.shape[0] // 2)
    before = jnp.dot(first_layer.T, embed, precision=exact)
    basis, slope = sincos(before)
    fraction = positions.astype(jnp.float32) / length
    window = jnp.exp(-rates[:, None] * fraction[None, :])
    shaped = window * jnp.dot(columns.T, basis, precision=precise)
    norms = jnp.sqrt(jnp.sum(shaped * shaped, axis=1, keepdims=True) + epsilon)
    filt = shaped / norms
    taps = tiled(filt + jnp.where(positions[None, :] == 0, gains[:, None], 0.0))
    cot, signal, taps, basis, slope = lax.optimization_barrier((cot, signal, taps, basis, slope))
    val = spread(signal)
    in_grad = correlate(taps, cot, cot.shape, group, "input_grad", tabs)
    val, in_grad = lax.optimization_barrier((val, in_grad))
    input_grad = lax.all_to_all(in_grad, "batch", split_axis=0, concat_axis=0, tiled=True)
    filt_grad = correlate(val, cot, taps.shape, group, "filter_grad", tabs)
    input_grad = input_grad.reshape(parts, groups, local_len // LANES, group, LANES)
    input_grad = input_grad.transpose(0, 1, 3, 2, 4).reshape(width_dev, local_len)
    filt_grad = filt_grad.reshape(groups, rows, group, LANES).transpose(0, 2, 1, 3)
    dfilt = factor * filt_grad.reshape(narrow, length)
    skip_part = (cot * val).reshape(parts, groups, local_len // LANES, group, LANES)
    skip_part = factor * jnp.sum(skip_part, axis=(0, 2, 4)).reshape(narrow)
    project = jnp.sum(filt * dfilt, axis=1, keepdims=True)
    draw = (dfilt - filt * project) / norms
    decay_part = -jnp.sum(draw * shaped * fraction[None, :], axis=1)
    dmix = draw * window
    second_part = jnp.dot(dmix, basis.T, precision=precise)
    dbasis = jnp.dot(columns, dmix, precision=precise)
    first_part = jnp.dot(embed, (slope * dbasis).T, precision=precise)
    bands, order = first_layer.shape
    left = jnp.concatenate([decay_part, skip_part])
    left = jnp.concatenate([first_part, jnp.pad(left, (0, order - 2 * narrow))[None]], axis=0)
    high = -(-max(bands + 1, narrow) // 8) * 8
    left = jnp.pad(left, ((0, high - bands - 1), (0, 0)))
    right = jnp.pad(second_part, ((0, high - narrow), (0, 0)))
    block = jnp.concatenate([left, right], axis=1)
    block, input_grad = lax.optimization_barrier((block, input_grad))
    shared, total = share(block, parts, lax.axis_size("chan"))
    first_grad = total[:bands, :order]
    second_grad = shared[:, :narrow, order:].reshape(width_dev, order).T
    decay_grad = shared[:, bands, :narrow].reshape(width_dev)
    skip_grad = shared[:, bands, narrow : 2 * narrow].reshape(width_dev)
    return (input_grad, first_grad, second_grad, decay_grad, skip_grad)


def solution(mesh):
    placed = (P("chan", "batch"), P("chan", "batch"), P(), P(None, "chan"), P("chan"), P("chan"))
    return jax.shard_map(
        local,
        mesh=mesh,
        in_specs=placed,
        out_specs=(P("chan", "batch"), P(), P(None, "chan"), P("chan"), P("chan")),
        check_vma=False,
    )
```

```python
import functools
import math

import jax
import jax.numpy as jnp
import numpy as np
from jax import lax
from jax.experimental import pallas as pl
from jax.experimental.pallas import tpu as pltpu
from jax.sharding import PartitionSpec as P

LANES = 128

exact = lax.Precision.HIGHEST
precise = lax.Precision.HIGH
epsilon = 1e-06


def sincos(x):
    turns = jnp.round(x * (2.0 / math.pi))
    r = x - turns * 1.5703125
    r = r - turns * 4.837512969970703125e-4
    r = r - turns * 7.549789948768648e-8
    sq = r * r
    sine = r + r * sq * (-1.6666654611e-1 + sq * (8.3321608736e-3 + sq * -1.9515295891e-4))
    cosine = 1.0 - 0.5 * sq + sq * sq * (
        4.166664568298827e-2 + sq * (-1.388731625493765e-3 + sq * 2.443315711809948e-5)
    )
    quadrant = turns.astype(jnp.int32) & 3
    odd = (quadrant & 1) == 1
    sin_value = jnp.where(odd, cosine, sine)
    cos_value = jnp.where(odd, sine, cosine)
    sin_value = jnp.where(quadrant >= 2, -sin_value, sin_value)
    cos_value = jnp.where((quadrant == 1) | (quadrant == 2), -cos_value, cos_value)
    return sin_value, cos_value


def pair(matrix):
    high = matrix.astype(np.float32).astype(jnp.bfloat16)
    low = (matrix - high.astype(np.float64)).astype(np.float32).astype(jnp.bfloat16)
    return jnp.asarray(high), jnp.asarray(low)


def tables(rows, cols):
    r = np.arange(rows, dtype=np.float64)
    c = np.arange(cols, dtype=np.float64)
    first = 2.0 * np.pi * np.outer(r + 0.5, r) / (2 * rows)
    twist = 2.0 * np.pi * np.outer(r + 0.5, c) / (2 * rows * cols)
    angle = 2.0 * np.pi * (np.outer(c, c) % cols) / cols
    cos_c, sin_c = np.cos(angle), np.sin(angle)
    stage1 = np.concatenate([np.cos(first), -np.sin(first)], axis=0)
    stage2 = np.block([[cos_c, -sin_c], [sin_c, cos_c]])
    last = np.concatenate([np.cos(first.T), -np.sin(first.T)], axis=1) / (rows * cols)
    return (
        *pair(stage1),
        *pair(stage2),
        *pair(stage2.T.copy()),
        *pair(last),
        jnp.asarray(np.cos(twist), jnp.float32),
        jnp.asarray(np.sin(twist), jnp.float32),
    )


def split(x):
    high = x.astype(jnp.bfloat16)
    return high, (x - high.astype(jnp.float32)).astype(jnp.bfloat16)


def dot(a, b):
    return jnp.dot(a, b, preferred_element_type=jnp.float32)


def product(left, right):
    return dot(left[0], right[0]) + (dot(left[1], right[0]) + dot(left[0], right[1]))


def forward(arrays, first, second, cos_t, sin_t):
    rows, cols = cos_t.shape
    t = product(first, split(jnp.concatenate(arrays, axis=1)))
    parts = []
    for i in range(len(arrays)):
        re = t[:rows, i * cols : (i + 1) * cols]
        im = t[rows:, i * cols : (i + 1) * cols]
        parts.append(jnp.concatenate([re * cos_t + im * sin_t, im * cos_t - re * sin_t], axis=1))
    spec = product(split(jnp.concatenate(parts, axis=0)), second)
    return [
        (spec[i * rows : (i + 1) * rows, :cols], spec[i * rows : (i + 1) * rows, cols:])
        for i in range(len(arrays))
    ]


def backward(spectra, third, last, cos_t, sin_t):
    rows, cols = cos_t.shape
    prods = jnp.concatenate([jnp.concatenate(s, axis=1) for s in spectra], axis=0)
    back = product(split(prods), third)
    turns = []
    for i in range(len(spectra)):
        re, im = back[i * rows : (i + 1) * rows, :cols], back[i * rows : (i + 1) * rows, cols:]
        turns.append(
            jnp.concatenate([re * cos_t - im * sin_t, im * cos_t + re * sin_t], axis=0)
        )
    out = product(last, split(jnp.concatenate(turns, axis=1)))
    return [out[:, i * cols : (i + 1) * cols] for i in range(len(spectra))]


def channel(ref, chunk, lane, group):
    count = ref.shape[2] // group
    return jnp.concatenate(
        [ref[b, chunk, pl.ds(lane, count, stride=group), :] for b in range(ref.shape[0])], axis=0
    )


def put(ref, chunk, lane, group, value):
    count = ref.shape[2] // group
    for b in range(ref.shape[0]):
        ref[b, chunk, pl.ds(lane, count, stride=group), :] = value[b * count : (b + 1) * count]


def conjugate(left, right):
    (a_re, a_im), (b_re, b_im) = left, right
    return a_re * b_re + a_im * b_im, a_re * b_im - a_im * b_re


MESH = pl.DeviceIdType.MESH


def share_kernel(parts, chans, mine, shared, total, slots, partial, sums, sends, arrivals, sends2, arrivals2):
    me, my_chan = lax.axis_index("batch"), lax.axis_index("chan")
    barrier = pltpu.get_barrier_semaphore()
    for k in range(1, parts):
        peer = lax.rem(me + k, parts)
        pl.semaphore_signal(barrier, inc=1, device_id=(peer, my_chan), device_id_type=MESH)
    for k in range(1, chans):
        peer = lax.rem(my_chan + k, chans)
        pl.semaphore_signal(barrier, inc=1, device_id=(me, peer), device_id_type=MESH)
    pl.semaphore_wait(barrier, parts + chans - 2)
    copies = []
    for k in range(1, parts):
        copies.append(
            pltpu.make_async_remote_copy(
                src_ref=mine,
                dst_ref=slots.at[k],
                send_sem=sends.at[k],
                recv_sem=arrivals.at[k],
                device_id=(lax.rem(me + k, parts), my_chan),
                device_id_type=MESH,
            )
        )
        copies[-1].start()
    slots[0] = mine[...]
    for copy in copies:
        copy.wait_recv()
    acc = jnp.zeros(mine.shape, jnp.float32)
    for b in range(parts):
        block = slots[lax.rem(me + parts - b, parts)]
        shared[b] = block
        acc = acc + block
    partial[...] = acc
    for copy in copies:
        copy.wait_send()
    copies = []
    for k in range(1, chans):
        copies.append(
            pltpu.make_async_remote_copy(
                src_ref=partial,
                dst_ref=sums.at[k],
                send_sem=sends2.at[k],
                recv_sem=arrivals2.at[k],
                device_id=(me, lax.rem(my_chan + k, chans)),
                device_id_type=MESH,
            )
        )
        copies[-1].start()
    sums[0] = acc
    for copy in copies:
        copy.wait_recv()
    acc = jnp.zeros_like(acc)
    for c in range(chans):
        acc = acc + sums[lax.rem(my_chan + chans - c, chans)]
    total[...] = acc
    for copy in copies:
        copy.wait_send()


def share(block, parts, chans):
    vmem = pl.BlockSpec(memory_space=pltpu.VMEM)
    dma = pltpu.SemaphoreType.DMA
    return pl.pallas_call(
        functools.partial(share_kernel, parts, chans),
        in_specs=[vmem],
        out_specs=[vmem, vmem],
        out_shape=[
            jax.ShapeDtypeStruct((parts, *block.shape), jnp.float32),
            jax.ShapeDtypeStruct(block.shape, jnp.float32),
        ],
        scratch_shapes=[
            pltpu.VMEM((parts, *block.shape), jnp.float32),
            pltpu.VMEM(block.shape, jnp.float32),
            pltpu.VMEM((chans, *block.shape), jnp.float32),
            dma((parts,)),
            dma((parts,)),
            dma((chans,)),
            dma((chans,)),
        ],
        compiler_params=pltpu.CompilerParams(collective_id=0, has_side_effects=True),
        name="share",
    )(block)


def block_kernel(
    parts, group, nb, sig_in, cot_in, first_t, mix, rates, gains,
    w1h, w1l, w2h, w2l, w3h, w3l, w4h, w4l, ct, st,
    v1h, v1l, v4h, v4l, cv, sv,
    in_out, filt_out, raw_out, basis_out, slope_out, embed_out, norm_out,
    cot_buf, sig_buf, ig_buf, late_cot, late_sig, raw_buf, basis_buf, slope_buf, embed_buf,
    zero_buf, inverse,
    cot_got, sig_got, late_cot_got, late_sig_got, ig_got,
    cot_sent, sig_sent, late_sent, ig_sent, late_ig_sent, done,
):
    me, my_chan = lax.axis_index("batch"), lax.axis_index("chan")
    half = parts // 2
    late = me >= half
    groups = cot_buf.shape[1]
    length = basis_buf.shape[1]
    padded = groups * 8
    barrier = pltpu.get_barrier_semaphore()
    for k in range(1, parts):
        peer = lax.rem(me + k, parts)
        pl.semaphore_signal(barrier, inc=1, device_id=(peer, my_chan), device_id_type=MESH)
    pl.semaphore_wait(barrier, parts - 1)

    def send(src, dst, sent, got, peer):
        pltpu.make_async_remote_copy(
            src_ref=src,
            dst_ref=dst,
            send_sem=sent,
            recv_sem=got,
            device_id=(peer, my_chan),
            device_id_type=MESH,
        ).start()

    def settle(ref, sem):
        pltpu.make_async_copy(ref, ref, sem).wait()

    for g in range(groups):
        pltpu.make_async_copy(cot_in.at[me, g], cot_buf.at[me, g], cot_got.at[g]).start()
        pltpu.make_async_copy(sig_in.at[me, g], sig_buf.at[me, g], sig_got.at[g]).start()

    @pl.when(late)
    def _():
        own = me - half
        for g in range(groups):
            pltpu.make_async_copy(cot_in.at[own, g], late_cot.at[own, g], late_cot_got.at[g]).start()
            pltpu.make_async_copy(sig_in.at[own, g], late_sig.at[own, g], late_sig_got.at[g]).start()
            for k in range(1, half):
                to = lax.rem(own + k, half)
                send(cot_in.at[to, g], late_cot.at[own, g], late_sent, late_cot_got.at[g], to + half)
                send(sig_in.at[to, g], late_sig.at[own, g], late_sent, late_sig_got.at[g], to + half)
            for k in range(1, parts):
                to = lax.rem(me + k, parts)
                send(cot_in.at[to, g], cot_buf.at[me, g], cot_sent, cot_got.at[g], to)
        for g in range(groups):
            for k in range(1, half):
                to = lax.rem(own + k, half) + half
                send(sig_in.at[to, g], sig_buf.at[me, g], sig_sent, sig_got.at[g], to)

    @pl.when(jnp.logical_not(late))
    def _():
        for g in range(groups):
            for k in range(1, parts):
                to = lax.rem(me + k, parts)
                send(cot_in.at[to, g], cot_buf.at[me, g], cot_sent, cot_got.at[g], to)
        for g in range(groups):
            for k in range(1, parts):
                to = lax.rem(me + k, parts)
                send(sig_in.at[to, g], sig_buf.at[me, g], sig_sent, sig_got.at[g], to)
        sig_buf[half:] = jnp.zeros((parts - half, *sig_buf.shape[1:]), jnp.float32)

    zero_buf[...] = jnp.zeros(zero_buf.shape, jnp.float32)

    other = lax.rem(me + half, parts)
    mine = pl.ds(pl.multiple_of(me * padded, 8), padded)
    theirs = pl.ds(pl.multiple_of(other * padded, 8), padded)
    weights = split(jnp.concatenate([mix[mine, :], mix[theirs, :]], axis=0))
    rate = jnp.concatenate([rates[mine, :], rates[theirs, :]], axis=0)[:, :1]
    tile = 512 if length % 512 == 0 else LANES
    width = tile // LANES

    def generate(t, total):
        start = pl.multiple_of(t * tile, tile)
        spot = (start + lax.broadcasted_iota(jnp.int32, (nb, tile), 1)).astype(jnp.float32)
        band = (lax.broadcasted_iota(jnp.int32, (nb, tile), 0) + 1).astype(jnp.float32)
        turn = band * spot * (1.0 / length)
        sines, cosines = sincos((turn - jnp.floor(turn)) * (2.0 * math.pi))
        line = (start + lax.broadcasted_iota(jnp.int32, (8, tile), 1)).astype(jnp.float32) / length
        line = jnp.where(lax.broadcasted_iota(jnp.int32, (8, tile), 0) == 0, line, 0.0)
        embed = jnp.concatenate([cosines, sines, line], axis=0)
        before = jnp.dot(
            first_t[...], embed, precision=exact, preferred_element_type=jnp.float32
        )
        basis, slope = sincos(before)
        embed_buf[:, pl.ds(start, tile)] = embed
        basis_buf[:, pl.ds(start, tile)] = basis
        slope_buf[:, pl.ds(start, tile)] = slope
        raw = jnp.exp(-rate * line[:1]) * product(weights, split(basis))
        for j in range(width):
            piece = raw[:, j * LANES : (j + 1) * LANES]
            total = total + piece * piece
            row = pl.ds(pl.multiple_of((t * width + j) * 8, 8), 8)
            for h in range(2 * groups):
                raw_buf[h, row, :] = piece[h * 8 : (h + 1) * 8]
        return total

    total = lax.fori_loop(
        0, length // tile, generate, jnp.zeros((2 * padded, LANES), jnp.float32)
    )
    norm = jnp.sqrt(jnp.sum(total, axis=1, keepdims=True) + epsilon)
    norm_out[...] = jnp.broadcast_to(norm, norm_out.shape)
    inverse[...] = jnp.broadcast_to(1.0 / norm, inverse.shape)
    outputs = ((raw_buf, raw_out), (basis_buf, basis_out), (slope_buf, slope_out), (embed_buf, embed_out))
    for i, (src, dst) in enumerate(outputs):
        pltpu.make_async_copy(src, dst, done.at[i]).start()

    second, third = (w2h[...], w2l[...]), (w3h[...], w3l[...])
    count = 2 if group % 2 == 0 else 1
    pairs = group // count
    rows = raw_buf.shape[1] // 8

    @pl.when(late)
    def _():
        own = me - half
        first, last = (v1h[...], v1l[...]), (v4h[...], v4l[...])
        cos_t, sin_t = cv[...], sv[...]

        def chunk(g, carry):
            settle(late_cot.at[:, g], late_cot_got.at[g])
            settle(late_sig.at[:, g], late_sig_got.at[g])

            def step(p, carry):
                lanes = [p * count + j for j in range(count)]
                cots = [channel(late_cot, g, lane, group) for lane in lanes]
                sigs = [channel(late_sig, g, lane, group) for lane in lanes]
                raws = [
                    raw_buf[groups + g, pl.ds(lane, rows // 2, stride=8), :] for lane in lanes
                ]
                specs = forward(cots + sigs + raws, first, second, cos_t, sin_t)
                prods = [conjugate(specs[2 * count + j], specs[j]) for j in range(count)]
                prods += [conjugate(specs[count + j], specs[j]) for j in range(count)]
                values = backward(prods, third, last, cos_t, sin_t)
                for j, lane in enumerate(lanes):
                    at = pl.ds(padded + g * 8 + lane, 1)
                    gain = gains[pl.ds(other * padded + g * 8 + lane, 1), :]
                    put(late_cot, g, lane, group, values[j] * inverse[at, :] + gain * cots[j])
                    put(late_sig, g, lane, group, values[count + j])
                return carry

            lax.fori_loop(0, pairs, step, 0)
            pltpu.make_async_copy(late_cot.at[own, g], in_out.at[own, g], ig_got).start()
            for k in range(1, half):
                to = lax.rem(own + k, half)
                send(late_cot.at[to, g], in_out.at[own, g], late_ig_sent, ig_got, to + half)
            pltpu.make_async_copy(late_sig.at[:, g], filt_out.at[groups + g, pl.ds(0, half)], done.at[4]).start()
            pltpu.make_async_copy(zero_buf, filt_out.at[groups + g, pl.ds(half, half)], done.at[5]).start()
            return carry

        lax.fori_loop(0, groups, chunk, 0)

    @pl.when(jnp.logical_not(late))
    def _():
        for g in range(groups):
            pltpu.make_async_copy(zero_buf, filt_out.at[groups + g, pl.ds(0, half)], done.at[4]).start()
            pltpu.make_async_copy(zero_buf, filt_out.at[groups + g, pl.ds(half, half)], done.at[5]).start()

    first, last = (w1h[...], w1l[...]), (w4h[...], w4l[...])
    cos_t, sin_t = ct[...], st[...]

    def input_chunk(g, carry):
        settle(cot_buf.at[:, g], cot_got.at[g])

        def step(p, carry):
            lanes = [p * count + j for j in range(count)]
            cots = [channel(cot_buf, g, lane, group) for lane in lanes]
            raws = [raw_buf[g, pl.ds(lane, rows, stride=8), :] for lane in lanes]
            specs = forward(raws + cots, first, second, cos_t, sin_t)
            prods = [conjugate(specs[j], specs[count + j]) for j in range(count)]
            values = backward(prods, third, last, cos_t, sin_t)
            for j, lane in enumerate(lanes):
                gain = gains[pl.ds(me * padded + g * 8 + lane, 1), :]
                scale = inverse[pl.ds(g * 8 + lane, 1), :]
                put(ig_buf, g, lane, group, values[j] * scale + gain * cots[j])
            return carry

        lax.fori_loop(0, pairs, step, 0)
        pltpu.make_async_copy(ig_buf.at[me, g], in_out.at[me, g], ig_got).start()

        @pl.when(late)
        def _():
            for k in range(1, parts):
                to = lax.rem(me + k, parts)
                send(ig_buf.at[to, g], in_out.at[me, g], ig_sent, ig_got, to)

        @pl.when(jnp.logical_not(late))
        def _():
            for k in range(1, half):
                to = lax.rem(me + k, half)
                send(ig_buf.at[to, g], in_out.at[me, g], ig_sent, ig_got, to)

        return carry

    lax.fori_loop(0, groups, input_chunk, 0)

    def filter_chunk(g, carry):
        @pl.when(late)
        def _():
            settle(sig_buf.at[:, g], sig_got.at[g])

        @pl.when(jnp.logical_not(late))
        def _():
            settle(sig_buf.at[pl.ds(0, half), g], sig_got.at[g])

        def step(p, carry):
            lanes = [p * count + j for j in range(count)]
            cots = [channel(cot_buf, g, lane, group) for lane in lanes]
            sigs = [channel(sig_buf, g, lane, group) for lane in lanes]
            specs = forward(sigs + cots, first, second, cos_t, sin_t)
            prods = [conjugate(specs[j], specs[count + j]) for j in range(count)]
            values = backward(prods, third, last, cos_t, sin_t)
            for j, lane in enumerate(lanes):
                put(sig_buf, g, lane, group, values[j])
            return carry

        lax.fori_loop(0, pairs, step, 0)
        pltpu.make_async_copy(sig_buf.at[:, g], filt_out.at[g], done.at[6]).start()
        return carry

    lax.fori_loop(0, groups, filter_chunk, 0)

    for i, (src, dst) in enumerate(outputs):
        settle(dst, done.at[i])
    settle(filt_out.at[pl.ds(0, groups), pl.ds(0, half)], done.at[4])
    settle(filt_out.at[pl.ds(0, groups), pl.ds(0, half)], done.at[5])
    settle(filt_out.at[pl.ds(0, groups)], done.at[6])
    settle(cot_in.at[pl.ds(0, parts - 1)], cot_sent)
    settle(in_out, ig_got)

    @pl.when(late)
    def _():
        settle(cot_in.at[pl.ds(0, 2 * (half - 1))], late_sent)
        settle(cot_in.at[pl.ds(0, half - 1)], late_ig_sent)
        settle(cot_in.at[pl.ds(0, half - 1)], sig_sent)
        settle(cot_in.at[pl.ds(0, parts - 1)], ig_sent)

    @pl.when(jnp.logical_not(late))
    def _():
        settle(cot_in.at[pl.ds(0, parts - 1)], sig_sent)
        settle(cot_in.at[pl.ds(0, half - 1)], ig_sent)


def run_block(sig, cot, first_t, mix, rates, gains, group, length):
    parts, groups, run, _ = sig.shape
    half = parts // 2
    rows = length // LANES
    nb = (first_t.shape[1] - 8) // 2
    order = first_t.shape[0]
    tabs = tables(rows, LANES)
    small = tables(rows // 2, LANES)
    small = (*small[:2], *small[6:])
    hbm = pl.BlockSpec(memory_space=pl.ANY)
    vmem = pl.BlockSpec(memory_space=pltpu.VMEM)
    dma = pltpu.SemaphoreType.DMA
    f32 = jnp.float32
    pieces = (first_t, mix, rates, gains, *tabs, *small)
    return pl.pallas_call(
        functools.partial(block_kernel, parts, group, nb),
        in_specs=[hbm, hbm] + [vmem] * len(pieces),
        out_specs=[hbm] * 6 + [vmem],
        out_shape=[
            jax.ShapeDtypeStruct(sig.shape, f32),
            jax.ShapeDtypeStruct((2 * groups, parts, run, LANES), f32),
            jax.ShapeDtypeStruct((2 * groups, rows * 8, LANES), f32),
            jax.ShapeDtypeStruct((order, length), f32),
            jax.ShapeDtypeStruct((order, length), f32),
            jax.ShapeDtypeStruct((first_t.shape[1], length), f32),
            jax.ShapeDtypeStruct((2 * groups * 8, LANES), f32),
        ],
        scratch_shapes=[
            pltpu.VMEM(sig.shape, f32),
            pltpu.VMEM(sig.shape, f32),
            pltpu.VMEM(sig.shape, f32),
            pltpu.VMEM((half, groups, run, LANES), f32),
            pltpu.VMEM((half, groups, run, LANES), f32),
            pltpu.VMEM((2 * groups, rows * 8, LANES), f32),
            pltpu.VMEM((order, length), f32),
            pltpu.VMEM((order, length), f32),
            pltpu.VMEM((first_t.shape[1], length), f32),
            pltpu.VMEM((half, run, LANES), f32),
            pltpu.VMEM((2 * groups * 8, LANES), f32),
            dma((groups,)),
            dma((groups,)),
            dma((groups,)),
            dma((groups,)),
            dma,
            dma,
            dma,
            dma,
            dma,
            dma,
            dma((7,)),
        ],
        compiler_params=pltpu.CompilerParams(
            collective_id=1, has_side_effects=True, vmem_limit_bytes=67043328
        ),
        name="block",
    )(sig, cot, *pieces)


def local(signal, cotangent, first_layer, second_layer, decay_rate, skip_gain):
    parts = lax.axis_size("batch")
    place = lax.axis_index("batch")
    width_dev, local_len = signal.shape
    bands, order = first_layer.shape
    length = local_len * parts
    factor = 1.0 / math.sqrt(length)
    narrow = width_dev // parts
    group = min(8, narrow)
    groups = narrow // group
    rows = length // LANES
    nb = bands // 2

    def tiles(x):
        x = x.reshape(parts, groups, group, local_len // LANES, LANES)
        return x.transpose(0, 1, 3, 2, 4).reshape(parts, groups, -1, LANES)

    def fill(x):
        x = x.reshape(parts * groups, group, -1)
        x = jnp.pad(x, ((0, 0), (0, 8 - group), (0, 0)))
        return x.reshape(parts * groups * 8, -1)

    first_t = jnp.concatenate([first_layer[1:], first_layer[:1]], axis=0)
    first_t = jnp.pad(first_t, ((0, 7), (0, 0))).T
    spread = lambda x: jnp.broadcast_to(fill(x), (parts * groups * 8, LANES))
    in_grad, filt_grad, shaped, basis, slope, embed, norms = run_block(
        tiles(signal),
        tiles(cotangent),
        first_t,
        fill(second_layer.T),
        spread(decay_rate),
        spread(skip_gain),
        group,
        length,
    )
    input_grad = in_grad.reshape(parts, groups, local_len // LANES, group, LANES)
    input_grad = input_grad.transpose(0, 1, 3, 2, 4).reshape(width_dev, local_len)

    def flat(x, q):
        x = x.reshape(2 * groups, rows, q, LANES).transpose(0, 2, 1, 3)[:, :group]
        return x.reshape(2 * narrow, length)

    other = (place + parts // 2) % parts

    def both(x):
        own = lax.dynamic_slice_in_dim(x, place * narrow, narrow, 0)
        return jnp.concatenate([own, lax.dynamic_slice_in_dim(x, other * narrow, narrow, 0)])

    columns = both(second_layer.T).T
    rates = both(decay_rate)
    norms = norms.reshape(2 * groups, 8, LANES)[:, :group, :1].reshape(2 * narrow, 1)
    fraction = jnp.arange(length, dtype=jnp.int32).astype(jnp.float32) / length
    window = jnp.exp(-rates[:, None] * fraction[None, :])
    dfilt = factor * flat(filt_grad, group)
    shaped = flat(shaped, 8)
    filt = shaped / norms
    project = jnp.sum(filt * dfilt, axis=1, keepdims=True)
    draw = (dfilt - filt * project) / norms
    decay_part = -jnp.sum(draw * shaped * fraction[None, :], axis=1)
    dmix = draw * window
    second_part = jnp.dot(dmix, basis.T, precision=precise)
    dbasis = jnp.dot(columns, dmix, precision=precise)
    first_part = jnp.dot(embed, (slope * dbasis).T, precision=precise)
    skip_part = factor * jnp.sum(cotangent * signal, axis=1)
    left = jnp.concatenate(
        [
            first_part[2 * nb : bands],
            first_part[: 2 * nb],
            jnp.pad(decay_part, (0, order - 2 * narrow))[None],
            skip_part.reshape(-1, order),
        ],
        axis=0,
    )
    high = -(-max(left.shape[0], 2 * narrow) // 8) * 8
    left = jnp.pad(left, ((0, high - left.shape[0]), (0, 0)))
    right = jnp.pad(second_part, ((0, high - 2 * narrow), (0, 0)))
    block = jnp.concatenate([left, right], axis=1)
    shared, total = share(block, parts, lax.axis_size("chan"))
    first_grad = total[:bands, :order]

    def merge(own, late):
        return own + jnp.roll(late, -(parts // 2), axis=0)

    second_grad = merge(shared[:, :narrow, order:], shared[:, narrow : 2 * narrow, order:])
    second_grad = second_grad.reshape(width_dev, order).T
    decays = shared[:, bands]
    decay_grad = merge(decays[:, :narrow], decays[:, narrow : 2 * narrow]).reshape(width_dev)
    skip_grad = jnp.sum(shared[:, bands + 1 : bands + 1 + width_dev // order, :order], axis=0)
    return (input_grad, first_grad, second_grad, decay_grad, skip_grad.reshape(width_dev))


def solution(mesh):
    placed = (P("chan", "batch"), P("chan", "batch"), P(), P(None, "chan"), P("chan"), P("chan"))
    return jax.shard_map(
        local,
        mesh=mesh,
        in_specs=placed,
        out_specs=(P("chan", "batch"), P(), P(None, "chan"), P("chan"), P("chan")),
        check_vma=False,
    )
```

```python
import functools
import math

import jax
import jax.numpy as jnp
import numpy as np
from jax import lax
from jax.experimental import pallas as pl
from jax.experimental.pallas import tpu as pltpu
from jax.sharding import PartitionSpec as P

LANES = 128

exact = lax.Precision.HIGHEST
precise = lax.Precision.HIGH
epsilon = 1e-06


def sincos(x):
    turns = jnp.round(x * (2.0 / math.pi))
    r = x - turns * 1.5703125
    r = r - turns * 4.837512969970703125e-4
    r = r - turns * 7.549789948768648e-8
    sq = r * r
    sine = r + r * sq * (-1.6666654611e-1 + sq * (8.3321608736e-3 + sq * -1.9515295891e-4))
    cosine = 1.0 - 0.5 * sq + sq * sq * (
        4.166664568298827e-2 + sq * (-1.388731625493765e-3 + sq * 2.443315711809948e-5)
    )
    quadrant = turns.astype(jnp.int32) & 3
    odd = (quadrant & 1) == 1
    sin_value = jnp.where(odd, cosine, sine)
    cos_value = jnp.where(odd, sine, cosine)
    sin_value = jnp.where(quadrant >= 2, -sin_value, sin_value)
    cos_value = jnp.where((quadrant == 1) | (quadrant == 2), -cos_value, cos_value)
    return sin_value, cos_value


def pair(matrix):
    high = matrix.astype(np.float32).astype(jnp.bfloat16)
    low = (matrix - high.astype(np.float64)).astype(np.float32).astype(jnp.bfloat16)
    return jnp.asarray(high), jnp.asarray(low)


def tables(rows, cols):
    r = np.arange(rows, dtype=np.float64)
    c = np.arange(cols, dtype=np.float64)
    first = 2.0 * np.pi * np.outer(r + 0.5, r) / (2 * rows)
    twist = 2.0 * np.pi * np.outer(r + 0.5, c) / (2 * rows * cols)
    angle = 2.0 * np.pi * (np.outer(c, c) % cols) / cols
    cos_c, sin_c = np.cos(angle), np.sin(angle)
    stage1 = np.concatenate([np.cos(first), -np.sin(first)], axis=0)
    stage2 = np.block([[cos_c, -sin_c], [sin_c, cos_c]])
    last = np.concatenate([np.cos(first.T), -np.sin(first.T)], axis=1) / (rows * cols)
    return (
        *pair(stage1),
        *pair(stage2),
        *pair(stage2.T.copy()),
        *pair(last),
        jnp.asarray(np.cos(twist), jnp.float32),
        jnp.asarray(np.sin(twist), jnp.float32),
    )


def split(x):
    high = x.astype(jnp.bfloat16)
    return high, (x - high.astype(jnp.float32)).astype(jnp.bfloat16)


def dot(a, b):
    return jnp.dot(a, b, preferred_element_type=jnp.float32)


def product(left, right):
    return dot(left[0], right[0]) + (dot(left[1], right[0]) + dot(left[0], right[1]))


def forward(arrays, first, second, cos_t, sin_t):
    rows, cols = cos_t.shape
    t = product(first, split(jnp.concatenate(arrays, axis=1)))
    parts = []
    for i in range(len(arrays)):
        re = t[:rows, i * cols : (i + 1) * cols]
        im = t[rows:, i * cols : (i + 1) * cols]
        parts.append(jnp.concatenate([re * cos_t + im * sin_t, im * cos_t - re * sin_t], axis=1))
    spec = product(split(jnp.concatenate(parts, axis=0)), second)
    return [
        (spec[i * rows : (i + 1) * rows, :cols], spec[i * rows : (i + 1) * rows, cols:])
        for i in range(len(arrays))
    ]


def backward(spectra, third, last, cos_t, sin_t):
    rows, cols = cos_t.shape
    prods = jnp.concatenate([jnp.concatenate(s, axis=1) for s in spectra], axis=0)
    back = product(split(prods), third)
    turns = []
    for i in range(len(spectra)):
        re, im = back[i * rows : (i + 1) * rows, :cols], back[i * rows : (i + 1) * rows, cols:]
        turns.append(
            jnp.concatenate([re * cos_t - im * sin_t, im * cos_t + re * sin_t], axis=0)
        )
    out = product(last, split(jnp.concatenate(turns, axis=1)))
    return [out[:, i * cols : (i + 1) * cols] for i in range(len(spectra))]


def channel(ref, chunk, lane, group):
    count = ref.shape[2] // group
    return jnp.concatenate(
        [ref[b, chunk, pl.ds(lane, count, stride=group), :] for b in range(ref.shape[0])], axis=0
    )


def put(ref, chunk, lane, group, value):
    count = ref.shape[2] // group
    for b in range(ref.shape[0]):
        ref[b, chunk, pl.ds(lane, count, stride=group), :] = value[b * count : (b + 1) * count]


def conjugate(left, right):
    (a_re, a_im), (b_re, b_im) = left, right
    return a_re * b_re + a_im * b_im, a_re * b_im - a_im * b_re


MESH = pl.DeviceIdType.MESH


def block_kernel(
    parts, chans, group, nb, sig_in, cot_in, first_t, mix, mix_t, rates, gains,
    w1h, w1l, w2h, w2l, w3h, w3l, w4h, w4l, ct, st,
    v1h, v1l, v4h, v4l, cv, sv,
    in_out, shared, whole,
    cot_buf, sig_buf, ig_buf, late_cot, late_sig, raw_buf, basis_buf, slope_buf, embed_buf,
    inverse, project, skip, decay, second_buf, first_buf, mine_buf, slots, partial, sums,
    cot_got, sig_got, late_cot_got, late_sig_got, ig_got,
    cot_sent, sig_sent, late_sent, ig_sent, late_ig_sent, sends, arrivals, sends2, arrivals2,
):
    me, my_chan = lax.axis_index("batch"), lax.axis_index("chan")
    half = parts // 2
    late = me >= half
    groups = cot_buf.shape[1]
    length = basis_buf.shape[1]
    padded = groups * 8
    barrier = pltpu.get_barrier_semaphore()
    for k in range(1, parts):
        peer = lax.rem(me + k, parts)
        pl.semaphore_signal(barrier, inc=1, device_id=(peer, my_chan), device_id_type=MESH)
    for k in range(1, chans):
        peer = lax.rem(my_chan + k, chans)
        pl.semaphore_signal(barrier, inc=1, device_id=(me, peer), device_id_type=MESH)
    pl.semaphore_wait(barrier, parts + chans - 2)

    def send(src, dst, sent, got, peer):
        pltpu.make_async_remote_copy(
            src_ref=src,
            dst_ref=dst,
            send_sem=sent,
            recv_sem=got,
            device_id=(peer, my_chan),
            device_id_type=MESH,
        ).start()

    def settle(ref, sem):
        pltpu.make_async_copy(ref, ref, sem).wait()

    for g in range(groups):
        pltpu.make_async_copy(cot_in.at[me, g], cot_buf.at[me, g], cot_got.at[g]).start()
        pltpu.make_async_copy(sig_in.at[me, g], sig_buf.at[me, g], sig_got.at[g]).start()

    @pl.when(late)
    def _():
        own = me - half
        for g in range(groups):
            pltpu.make_async_copy(cot_in.at[own, g], late_cot.at[own, g], late_cot_got.at[g]).start()
            pltpu.make_async_copy(sig_in.at[own, g], late_sig.at[own, g], late_sig_got.at[g]).start()
            for k in range(1, half):
                to = lax.rem(own + k, half)
                send(cot_in.at[to, g], late_cot.at[own, g], late_sent, late_cot_got.at[g], to + half)
                send(sig_in.at[to, g], late_sig.at[own, g], late_sent, late_sig_got.at[g], to + half)
            for k in range(1, parts):
                to = lax.rem(me + k, parts)
                send(cot_in.at[to, g], cot_buf.at[me, g], cot_sent, cot_got.at[g], to)
        for g in range(groups):
            for k in range(1, half):
                to = lax.rem(own + k, half) + half
                send(sig_in.at[to, g], sig_buf.at[me, g], sig_sent, sig_got.at[g], to)

    @pl.when(jnp.logical_not(late))
    def _():
        for g in range(groups):
            for k in range(1, parts):
                to = lax.rem(me + k, parts)
                send(cot_in.at[to, g], cot_buf.at[me, g], cot_sent, cot_got.at[g], to)
        for g in range(groups):
            for k in range(1, parts):
                to = lax.rem(me + k, parts)
                send(sig_in.at[to, g], sig_buf.at[me, g], sig_sent, sig_got.at[g], to)
        sig_buf[half:] = jnp.zeros((parts - half, *sig_buf.shape[1:]), jnp.float32)

    skip[...] = jnp.zeros(skip.shape, jnp.float32)
    project[...] = jnp.zeros(project.shape, jnp.float32)
    decay[...] = jnp.zeros(decay.shape, jnp.float32)
    second_buf[...] = jnp.zeros(second_buf.shape, jnp.float32)
    first_buf[...] = jnp.zeros(first_buf.shape, jnp.float32)
    other = lax.rem(me + half, parts)
    mine = pl.ds(pl.multiple_of(me * padded, 8), padded)
    theirs = pl.ds(pl.multiple_of(other * padded, 8), padded)
    weights = split(jnp.concatenate([mix[mine, :], mix[theirs, :]], axis=0))
    rate = jnp.concatenate([rates[mine, :], rates[theirs, :]], axis=0)[:, :1]
    tile = 512 if length % 512 == 0 else LANES
    width = tile // LANES

    def generate(t, total):
        start = pl.multiple_of(t * tile, tile)
        spot = (start + lax.broadcasted_iota(jnp.int32, (nb, tile), 1)).astype(jnp.float32)
        band = (lax.broadcasted_iota(jnp.int32, (nb, tile), 0) + 1).astype(jnp.float32)
        turn = band * spot * (1.0 / length)
        sines, cosines = sincos((turn - jnp.floor(turn)) * (2.0 * math.pi))
        line = (start + lax.broadcasted_iota(jnp.int32, (8, tile), 1)).astype(jnp.float32) / length
        line = jnp.where(lax.broadcasted_iota(jnp.int32, (8, tile), 0) == 0, line, 0.0)
        embed = jnp.concatenate([cosines, sines, line], axis=0)
        before = jnp.dot(
            first_t[...], embed, precision=exact, preferred_element_type=jnp.float32
        )
        basis, slope = sincos(before)
        embed_buf[:, pl.ds(start, tile)] = embed
        basis_buf[:, pl.ds(start, tile)] = basis
        slope_buf[:, pl.ds(start, tile)] = slope
        raw = jnp.exp(-rate * line[:1]) * product(weights, split(basis))
        for j in range(width):
            piece = raw[:, j * LANES : (j + 1) * LANES]
            total = total + piece * piece
            row = pl.ds(pl.multiple_of((t * width + j) * 8, 8), 8)
            for h in range(2 * groups):
                raw_buf[h, row, :] = piece[h * 8 : (h + 1) * 8]
        return total

    total = lax.fori_loop(
        0, length // tile, generate, jnp.zeros((2 * padded, LANES), jnp.float32)
    )
    norm = jnp.sqrt(jnp.sum(total, axis=1, keepdims=True) + epsilon)
    inverse[...] = jnp.broadcast_to(1.0 / norm, inverse.shape)
    factor = 1.0 / math.sqrt(length)
    long = 1024 if length % 1024 == 0 else LANES

    def total_of(ref, base):
        return jnp.sum(ref[pl.ds(base, padded), :], axis=1, keepdims=True)

    def functionals(lags, base, weights_t):
        scale = inverse[pl.ds(base, padded), :][:, :1]
        weight = factor * scale
        shift = -weight * scale * scale * total_of(project, base)
        speed = rate[base : base + padded]
        mixer = split(weights_t)
        per = long // LANES
        run = lags.shape[2] // group
        first_chunk = base // 8

        def gather(t, fetch):
            lines = []
            for h in range(groups):
                lines.append(jnp.concatenate([fetch(h, t * per + j) for j in range(per)], axis=1))
            return jnp.concatenate(lines, axis=0)

        def lag_tile(h, r):
            b = lax.div(r, run)
            at = (r - b * run) * group
            if group == 8:
                at = pl.multiple_of(at, 8)
            value = lags[b, h, pl.ds(at, group), :]
            if group < 8:
                value = jnp.concatenate(
                    [value, jnp.zeros((8 - group, LANES), jnp.float32)], axis=0
                )
            return value

        def raw_tile(h, r):
            return raw_buf[first_chunk + h, pl.ds(pl.multiple_of(r * 8, 8), 8), :]

        def nt(left, right):
            dims = (((1,), (1,)), ((), ()))
            one = lambda x, y: lax.dot_general(x, y, dims, preferred_element_type=jnp.float32)
            return one(left[0], right[0]) + (one(left[1], right[0]) + one(left[0], right[1]))

        def step(lagged, t, sums_so_far):
            second_sum, first_sum, decay_sum = sums_so_far
            start = pl.multiple_of(t * long, long)
            embed = embed_buf[:, pl.ds(start, long)]
            line = embed[2 * nb : 2 * nb + 1]
            raw = gather(t, raw_tile)
            draw = raw * shift
            if lagged:
                draw = draw + gather(t, lag_tile) * weight
            moment = draw * raw * line
            for j in range(per):
                decay_sum = decay_sum - moment[:, j * LANES : (j + 1) * LANES]
            dmix = split(draw * jnp.exp(-speed * line))
            second_sum = second_sum + nt(dmix, split(basis_buf[:, pl.ds(start, long)]))
            dbasis = product(mixer, dmix) * slope_buf[:, pl.ds(start, long)]
            first_sum = first_sum + nt(split(embed), split(dbasis))
            return second_sum, first_sum, decay_sum

        order = basis_buf.shape[0]
        state = (
            jnp.zeros((padded, order), jnp.float32),
            jnp.zeros((embed_buf.shape[0], order), jnp.float32),
            jnp.zeros((padded, LANES), jnp.float32),
        )
        covered, steps = lags.shape[0] * run // per, length // long
        state = lax.fori_loop(0, covered, functools.partial(step, True), state)
        if covered < steps:
            state = lax.fori_loop(covered, steps, functools.partial(step, False), state)
        second_sum, first_sum, decay_sum = state
        second_buf[base : base + padded] = second_sum
        first_buf[...] = first_buf[...] + first_sum
        decay[base : base + padded] = decay_sum

    second, third = (w2h[...], w2l[...]), (w3h[...], w3l[...])
    count = 2 if group % 2 == 0 else 1
    pairs = group // count
    rows = raw_buf.shape[1] // 8

    @pl.when(late)
    def _():
        own = me - half
        first, last = (v1h[...], v1l[...]), (v4h[...], v4l[...])
        cos_t, sin_t = cv[...], sv[...]

        def chunk(g, carry):
            settle(late_cot.at[:, g], late_cot_got.at[g])
            settle(late_sig.at[:, g], late_sig_got.at[g])

            def step(p, carry):
                lanes = [p * count + j for j in range(count)]
                cots = [channel(late_cot, g, lane, group) for lane in lanes]
                sigs = [channel(late_sig, g, lane, group) for lane in lanes]
                raws = [
                    raw_buf[groups + g, pl.ds(lane, rows // 2, stride=8), :] for lane in lanes
                ]
                specs = forward(cots + sigs + raws, first, second, cos_t, sin_t)
                prods = [conjugate(specs[2 * count + j], specs[j]) for j in range(count)]
                prods += [conjugate(specs[count + j], specs[j]) for j in range(count)]
                values = backward(prods, third, last, cos_t, sin_t)
                for j, lane in enumerate(lanes):
                    at = pl.ds(padded + g * 8 + lane, 1)
                    gain = gains[pl.ds(other * padded + g * 8 + lane, 1), :]
                    put(late_cot, g, lane, group, values[j] * inverse[at, :] + gain * cots[j])
                    put(late_sig, g, lane, group, values[count + j])
                    skip[at, :] = jnp.sum(cots[j] * sigs[j], axis=0, keepdims=True)
                    project[at, :] = jnp.sum(raws[j] * values[count + j], axis=0, keepdims=True)
                return carry

            lax.fori_loop(0, pairs, step, 0)
            pltpu.make_async_copy(late_cot.at[own, g], in_out.at[own, g], ig_got).start()
            for k in range(1, half):
                to = lax.rem(own + k, half)
                send(late_cot.at[to, g], in_out.at[own, g], late_ig_sent, ig_got, to + half)
            return carry

        lax.fori_loop(0, groups, chunk, 0)
        functionals(late_sig, padded, mix_t[own][:, :padded])

    first, last = (w1h[...], w1l[...]), (w4h[...], w4l[...])
    cos_t, sin_t = ct[...], st[...]

    def input_chunk(g, carry):
        settle(cot_buf.at[:, g], cot_got.at[g])

        def step(p, carry):
            lanes = [p * count + j for j in range(count)]
            cots = [channel(cot_buf, g, lane, group) for lane in lanes]
            raws = [raw_buf[g, pl.ds(lane, rows, stride=8), :] for lane in lanes]
            specs = forward(raws + cots, first, second, cos_t, sin_t)
            prods = [conjugate(specs[j], specs[count + j]) for j in range(count)]
            values = backward(prods, third, last, cos_t, sin_t)
            for j, lane in enumerate(lanes):
                gain = gains[pl.ds(me * padded + g * 8 + lane, 1), :]
                scale = inverse[pl.ds(g * 8 + lane, 1), :]
                put(ig_buf, g, lane, group, values[j] * scale + gain * cots[j])
            return carry

        lax.fori_loop(0, pairs, step, 0)
        pltpu.make_async_copy(ig_buf.at[me, g], in_out.at[me, g], ig_got).start()

        @pl.when(late)
        def _():
            for k in range(1, parts):
                to = lax.rem(me + k, parts)
                send(ig_buf.at[to, g], in_out.at[me, g], ig_sent, ig_got, to)

        @pl.when(jnp.logical_not(late))
        def _():
            for k in range(1, half):
                to = lax.rem(me + k, half)
                send(ig_buf.at[to, g], in_out.at[me, g], ig_sent, ig_got, to)

        return carry

    lax.fori_loop(0, groups, input_chunk, 0)

    def filter_chunk(g, carry):
        @pl.when(late)
        def _():
            settle(sig_buf.at[:, g], sig_got.at[g])

        @pl.when(jnp.logical_not(late))
        def _():
            settle(sig_buf.at[pl.ds(0, half), g], sig_got.at[g])

        def step(p, carry):
            lanes = [p * count + j for j in range(count)]
            cots = [channel(cot_buf, g, lane, group) for lane in lanes]
            sigs = [channel(sig_buf, g, lane, group) for lane in lanes]
            specs = forward(sigs + cots, first, second, cos_t, sin_t)
            prods = [conjugate(specs[j], specs[count + j]) for j in range(count)]
            values = backward(prods, third, last, cos_t, sin_t)
            for j, lane in enumerate(lanes):
                put(sig_buf, g, lane, group, values[j])
                at = pl.ds(g * 8 + lane, 1)
                raw = raw_buf[g, pl.ds(lane, rows, stride=8), :]
                skip[at, :] = jnp.sum(cots[j] * sigs[j], axis=0, keepdims=True)
                project[at, :] = jnp.sum(raw * values[j], axis=0, keepdims=True)
            return carry

        lax.fori_loop(0, pairs, step, 0)
        return carry

    lax.fori_loop(0, groups, filter_chunk, 0)

    functionals(sig_buf, 0, mix_t[me][:, :padded])

    def row_of(ref):
        column = jnp.sum(ref[...], axis=1, keepdims=True)
        shape = (2 * padded, LANES)
        same = lax.broadcasted_iota(jnp.int32, shape, 0) == lax.broadcasted_iota(jnp.int32, shape, 1)
        return jnp.sum(jnp.where(same, column, 0.0), axis=0, keepdims=True)

    order = basis_buf.shape[0]
    tall = embed_buf.shape[0]
    mine_buf[: 2 * padded, :order] = second_buf[...]
    mine_buf[:tall, order:] = first_buf[...]
    mine_buf[tall : tall + 1, order:] = row_of(decay)[:, :order]
    mine_buf[tall + 1 : tall + 2, order:] = factor * row_of(skip)[:, :order]

    copies = []
    for k in range(1, parts):
        copies.append(
            pltpu.make_async_remote_copy(
                src_ref=mine_buf,
                dst_ref=slots.at[k],
                send_sem=sends.at[k],
                recv_sem=arrivals.at[k],
                device_id=(lax.rem(me + k, parts), my_chan),
                device_id_type=MESH,
            )
        )
        copies[-1].start()
    slots[0] = mine_buf[...]
    for copy in copies:
        copy.wait_recv()
    acc = jnp.zeros(partial.shape, jnp.float32)
    for b in range(parts):
        block = slots[lax.rem(me + parts - b, parts)]
        shared[b] = block
        acc = acc + block[:tall]
    partial[...] = acc
    for copy in copies:
        copy.wait_send()
    copies = []
    for k in range(1, chans):
        copies.append(
            pltpu.make_async_remote_copy(
                src_ref=partial,
                dst_ref=sums.at[k],
                send_sem=sends2.at[k],
                recv_sem=arrivals2.at[k],
                device_id=(me, lax.rem(my_chan + k, chans)),
                device_id_type=MESH,
            )
        )
        copies[-1].start()
    sums[0] = acc
    for copy in copies:
        copy.wait_recv()
    acc = jnp.zeros_like(acc)
    for c in range(chans):
        acc = acc + sums[lax.rem(my_chan + chans - c, chans)]
    whole[...] = acc
    for copy in copies:
        copy.wait_send()

    settle(cot_in.at[pl.ds(0, parts - 1)], cot_sent)
    settle(in_out, ig_got)

    @pl.when(late)
    def _():
        settle(cot_in.at[pl.ds(0, 2 * (half - 1))], late_sent)
        settle(cot_in.at[pl.ds(0, half - 1)], late_ig_sent)
        settle(cot_in.at[pl.ds(0, half - 1)], sig_sent)
        settle(cot_in.at[pl.ds(0, parts - 1)], ig_sent)

    @pl.when(jnp.logical_not(late))
    def _():
        settle(cot_in.at[pl.ds(0, parts - 1)], sig_sent)
        settle(cot_in.at[pl.ds(0, half - 1)], ig_sent)


def run_block(sig, cot, first_t, mix, mix_t, rates, gains, group, length, chans):
    parts, groups, run, _ = sig.shape
    half = parts // 2
    rows = length // LANES
    nb = (first_t.shape[1] - 8) // 2
    order, tall = first_t.shape
    both = 2 * groups * 8
    high = -(-max(both, tall + 2) // 8) * 8
    tabs = tables(rows, LANES)
    small = tables(rows // 2, LANES)
    small = (*small[:2], *small[6:])
    hbm = pl.BlockSpec(memory_space=pl.ANY)
    vmem = pl.BlockSpec(memory_space=pltpu.VMEM)
    dma = pltpu.SemaphoreType.DMA
    f32 = jnp.float32
    pieces = (first_t, mix, mix_t, rates, gains, *tabs, *small)
    return pl.pallas_call(
        functools.partial(block_kernel, parts, chans, group, nb),
        in_specs=[hbm, hbm] + [vmem] * len(pieces),
        out_specs=[hbm, vmem, vmem],
        out_shape=[
            jax.ShapeDtypeStruct(sig.shape, f32),
            jax.ShapeDtypeStruct((parts, high, LANES), f32),
            jax.ShapeDtypeStruct((tall, LANES), f32),
        ],
        scratch_shapes=[
            pltpu.VMEM(sig.shape, f32),
            pltpu.VMEM(sig.shape, f32),
            pltpu.VMEM(sig.shape, f32),
            pltpu.VMEM((half, groups, run, LANES), f32),
            pltpu.VMEM((half, groups, run, LANES), f32),
            pltpu.VMEM((2 * groups, rows * 8, LANES), f32),
            pltpu.VMEM((order, length), f32),
            pltpu.VMEM((order, length), f32),
            pltpu.VMEM((tall, length), f32),
            pltpu.VMEM((both, LANES), f32),
            pltpu.VMEM((both, LANES), f32),
            pltpu.VMEM((both, LANES), f32),
            pltpu.VMEM((both, LANES), f32),
            pltpu.VMEM((both, order), f32),
            pltpu.VMEM((tall, order), f32),
            pltpu.VMEM((high, LANES), f32),
            pltpu.VMEM((parts, high, LANES), f32),
            pltpu.VMEM((tall, LANES), f32),
            pltpu.VMEM((chans, tall, LANES), f32),
            dma((groups,)),
            dma((groups,)),
            dma((groups,)),
            dma((groups,)),
            dma,
            dma,
            dma,
            dma,
            dma,
            dma,
            dma((parts,)),
            dma((parts,)),
            dma((chans,)),
            dma((chans,)),
        ],
        compiler_params=pltpu.CompilerParams(
            collective_id=1, has_side_effects=True, vmem_limit_bytes=67043328
        ),
        name="block",
    )(sig, cot, *pieces)


def local(signal, cotangent, first_layer, second_layer, decay_rate, skip_gain):
    parts = lax.axis_size("batch")
    width_dev, local_len = signal.shape
    bands, order = first_layer.shape
    length = local_len * parts
    narrow = width_dev // parts
    group = min(8, narrow)
    groups = narrow // group
    nb = bands // 2

    def tiles(x):
        x = x.reshape(parts, groups, group, local_len // LANES, LANES)
        return x.transpose(0, 1, 3, 2, 4).reshape(parts, groups, -1, LANES)

    def fill(x):
        x = x.reshape(parts * groups, group, -1)
        x = jnp.pad(x, ((0, 0), (0, 8 - group), (0, 0)))
        return x.reshape(parts * groups * 8, -1)

    first_t = jnp.concatenate([first_layer[1:], first_layer[:1]], axis=0)
    first_t = jnp.pad(first_t, ((0, 7), (0, 0))).T
    spread = lambda x: jnp.broadcast_to(fill(x), (parts * groups * 8, LANES))
    mix_t = fill(second_layer.T).reshape(parts, groups * 8, order).transpose(0, 2, 1)
    mix_t = jnp.pad(mix_t, ((0, 0), (0, 0), (0, max(0, LANES - groups * 8))))
    in_grad, shared, total = run_block(
        tiles(signal),
        tiles(cotangent),
        first_t,
        fill(second_layer.T),
        mix_t,
        spread(decay_rate),
        spread(skip_gain),
        group,
        length,
        lax.axis_size("chan"),
    )
    input_grad = in_grad.reshape(parts, groups, local_len // LANES, group, LANES)
    input_grad = input_grad.transpose(0, 1, 3, 2, 4).reshape(width_dev, local_len)
    first_grad = total[: bands + 7, order:]
    first_grad = jnp.concatenate([first_grad[2 * nb : bands], first_grad[: 2 * nb]], axis=0)

    def merge(x):
        own, late = x[:, : groups * 8], x[:, groups * 8 : 2 * groups * 8]
        x = own + jnp.roll(late, -(parts // 2), axis=0)
        x = x.reshape(parts, groups, 8, *x.shape[2:])[:, :, :group]
        return x.reshape(width_dev, *x.shape[3:])

    second_grad = merge(shared[:, :, :order]).T
    tall = bands + 7
    decay_grad = merge(shared[:, tall, order:])
    skip_grad = merge(shared[:, tall + 1, order:])
    return (input_grad, first_grad, second_grad, decay_grad, skip_grad)


def solution(mesh):
    placed = (P("chan", "batch"), P("chan", "batch"), P(), P(None, "chan"), P("chan"), P("chan"))
    return jax.shard_map(
        local,
        mesh=mesh,
        in_specs=placed,
        out_specs=(P("chan", "batch"), P(), P(None, "chan"), P("chan"), P("chan")),
        check_vma=False,
    )
```

```python
import functools
import math

import jax
import jax.numpy as jnp
import numpy as np
from jax import lax
from jax.experimental import pallas as pl
from jax.experimental.pallas import tpu as pltpu
from jax.sharding import PartitionSpec as P

LANES = 128

exact = lax.Precision.HIGHEST
precise = lax.Precision.HIGH
epsilon = 1e-06


def sincos(x):
    turns = jnp.round(x * (2.0 / math.pi))
    r = x - turns * 1.5703125
    r = r - turns * 4.837512969970703125e-4
    r = r - turns * 7.549789948768648e-8
    sq = r * r
    sine = r + r * sq * (-1.6666654611e-1 + sq * (8.3321608736e-3 + sq * -1.9515295891e-4))
    cosine = 1.0 - 0.5 * sq + sq * sq * (
        4.166664568298827e-2 + sq * (-1.388731625493765e-3 + sq * 2.443315711809948e-5)
    )
    quadrant = turns.astype(jnp.int32) & 3
    odd = (quadrant & 1) == 1
    sin_value = jnp.where(odd, cosine, sine)
    cos_value = jnp.where(odd, sine, cosine)
    sin_value = jnp.where(quadrant >= 2, -sin_value, sin_value)
    cos_value = jnp.where((quadrant == 1) | (quadrant == 2), -cos_value, cos_value)
    return sin_value, cos_value


def pair(matrix):
    high = matrix.astype(np.float32).astype(jnp.bfloat16)
    low = (matrix - high.astype(np.float64)).astype(np.float32).astype(jnp.bfloat16)
    return jnp.asarray(high), jnp.asarray(low)


def tables(rows, cols):
    r = np.arange(rows, dtype=np.float64)
    c = np.arange(cols, dtype=np.float64)
    first = 2.0 * np.pi * np.outer(r + 0.5, r) / (2 * rows)
    twist = 2.0 * np.pi * np.outer(r + 0.5, c) / (2 * rows * cols)
    angle = 2.0 * np.pi * (np.outer(c, c) % cols) / cols
    cos_c, sin_c = np.cos(angle), np.sin(angle)
    stage1 = np.concatenate([np.cos(first), -np.sin(first)], axis=0)
    stage2 = np.block([[cos_c, -sin_c], [sin_c, cos_c]])
    last = np.concatenate([np.cos(first.T), -np.sin(first.T)], axis=1) / (rows * cols)
    return (
        *pair(stage1),
        *pair(stage2),
        *pair(stage2.T.copy()),
        *pair(last),
        jnp.asarray(np.cos(twist), jnp.float32),
        jnp.asarray(np.sin(twist), jnp.float32),
    )


def split(x):
    high = x.astype(jnp.bfloat16)
    return high, (x - high.astype(jnp.float32)).astype(jnp.bfloat16)


def dot(a, b):
    return jnp.dot(a, b, preferred_element_type=jnp.float32)


def product(left, right):
    return dot(left[0], right[0]) + (dot(left[1], right[0]) + dot(left[0], right[1]))


def forward(arrays, first, second, cos_t, sin_t):
    rows, cols = cos_t.shape
    t = product(first, split(jnp.concatenate(arrays, axis=1)))
    parts = []
    for i in range(len(arrays)):
        re = t[:rows, i * cols : (i + 1) * cols]
        im = t[rows:, i * cols : (i + 1) * cols]
        parts.append(jnp.concatenate([re * cos_t + im * sin_t, im * cos_t - re * sin_t], axis=1))
    spec = product(split(jnp.concatenate(parts, axis=0)), second)
    return [
        (spec[i * rows : (i + 1) * rows, :cols], spec[i * rows : (i + 1) * rows, cols:])
        for i in range(len(arrays))
    ]


def backward(spectra, third, last, cos_t, sin_t):
    rows, cols = cos_t.shape
    prods = jnp.concatenate([jnp.concatenate(s, axis=1) for s in spectra], axis=0)
    back = product(split(prods), third)
    turns = []
    for i in range(len(spectra)):
        re, im = back[i * rows : (i + 1) * rows, :cols], back[i * rows : (i + 1) * rows, cols:]
        turns.append(
            jnp.concatenate([re * cos_t - im * sin_t, im * cos_t + re * sin_t], axis=0)
        )
    out = product(last, split(jnp.concatenate(turns, axis=1)))
    return [out[:, i * cols : (i + 1) * cols] for i in range(len(spectra))]


def channel(ref, chunk, lane, group):
    count = ref.shape[2] // group
    return jnp.concatenate(
        [ref[b, chunk, pl.ds(lane, count, stride=group), :] for b in range(ref.shape[0])], axis=0
    )


def put(ref, chunk, lane, group, value):
    count = ref.shape[2] // group
    for b in range(ref.shape[0]):
        ref[b, chunk, pl.ds(lane, count, stride=group), :] = value[b * count : (b + 1) * count]


def conjugate(left, right):
    (a_re, a_im), (b_re, b_im) = left, right
    return a_re * b_re + a_im * b_im, a_re * b_im - a_im * b_re


MESH = pl.DeviceIdType.MESH


def block_kernel(
    parts, chans, group, nb, sig_in, cot_in, first_t, layer, rates, gains,
    w1h, w1l, w2h, w2l, w3h, w3l, w4h, w4l, ct, st,
    v1h, v1l, v4h, v4l, cv, sv,
    in_out, turned, lines, whole,
    cot_buf, sig_buf, ig_buf, late_cot, late_sig, raw_buf, basis_buf, slope_buf, embed_buf,
    inverse, gain_buf, project, skip, late_msg, late_in, first_buf, mine_buf, slots, partial, sums,
    cot_got, sig_got, late_cot_got, late_sig_got, ig_got,
    cot_sent, sig_sent, late_sent, ig_sent, late_ig_sent, msg_sent, msg_got, sends, arrivals, sends2, arrivals2,
):
    me, my_chan = lax.axis_index("batch"), lax.axis_index("chan")
    half = parts // 2
    late = me >= half
    groups = cot_buf.shape[1]
    length = basis_buf.shape[1]
    padded = groups * 8
    barrier = pltpu.get_barrier_semaphore()
    for k in range(1, parts):
        peer = lax.rem(me + k, parts)
        pl.semaphore_signal(barrier, inc=1, device_id=(peer, my_chan), device_id_type=MESH)
    for k in range(1, chans):
        peer = lax.rem(my_chan + k, chans)
        pl.semaphore_signal(barrier, inc=1, device_id=(me, peer), device_id_type=MESH)
    pl.semaphore_wait(barrier, parts + chans - 2)

    def send(src, dst, sent, got, peer):
        pltpu.make_async_remote_copy(
            src_ref=src,
            dst_ref=dst,
            send_sem=sent,
            recv_sem=got,
            device_id=(peer, my_chan),
            device_id_type=MESH,
        ).start()

    def settle(ref, sem):
        pltpu.make_async_copy(ref, ref, sem).wait()

    for g in range(groups):
        pltpu.make_async_copy(cot_in.at[me, g], cot_buf.at[me, g], cot_got.at[g]).start()
        pltpu.make_async_copy(sig_in.at[me, g], sig_buf.at[me, g], sig_got.at[g]).start()

    @pl.when(late)
    def _():
        own = me - half
        for g in range(groups):
            pltpu.make_async_copy(cot_in.at[own, g], late_cot.at[own, g], late_cot_got.at[g]).start()
            pltpu.make_async_copy(sig_in.at[own, g], late_sig.at[own, g], late_sig_got.at[g]).start()
            for k in range(1, half):
                to = lax.rem(own + k, half)
                send(cot_in.at[to, g], late_cot.at[own, g], late_sent, late_cot_got.at[g], to + half)
                send(sig_in.at[to, g], late_sig.at[own, g], late_sent, late_sig_got.at[g], to + half)
            for k in range(1, parts):
                to = lax.rem(me + k, parts)
                send(cot_in.at[to, g], cot_buf.at[me, g], cot_sent, cot_got.at[g], to)
        for g in range(groups):
            for k in range(1, half):
                to = lax.rem(own + k, half) + half
                send(sig_in.at[to, g], sig_buf.at[me, g], sig_sent, sig_got.at[g], to)

    @pl.when(jnp.logical_not(late))
    def _():
        for g in range(groups):
            for k in range(1, parts):
                to = lax.rem(me + k, parts)
                send(cot_in.at[to, g], cot_buf.at[me, g], cot_sent, cot_got.at[g], to)
        for g in range(groups):
            for k in range(1, parts):
                to = lax.rem(me + k, parts)
                send(sig_in.at[to, g], sig_buf.at[me, g], sig_sent, sig_got.at[g], to)
        sig_buf[half:] = jnp.zeros((parts - half, *sig_buf.shape[1:]), jnp.float32)

    skip[...] = jnp.zeros(skip.shape, jnp.float32)
    project[...] = jnp.zeros(project.shape, jnp.float32)
    mine_buf[...] = jnp.zeros(mine_buf.shape, jnp.float32)
    first_buf[...] = jnp.zeros(first_buf.shape, jnp.float32)
    other = lax.rem(me + half, parts)
    wide = layer.shape[1]
    nt_dims = (((1,), (1,)), ((), ()))

    def pick(owner):
        line = lax.broadcasted_iota(jnp.int32, (padded, wide), 0)
        spot = owner * groups * group + lax.shift_right_logical(line, 3) * group + (line & 7)
        return jnp.logical_and(
            lax.broadcasted_iota(jnp.int32, (padded, wide), 1) == spot, (line & 7) < group
        )

    def column(mask, row):
        return jnp.sum(jnp.where(mask, row, 0.0), axis=1, keepdims=True)

    def exact_nt(left, right):
        return lax.dot_general(
            left, right, nt_dims, precision=exact, preferred_element_type=jnp.float32
        )

    masks = [pick(me), pick(other)]
    hots = [mask.astype(jnp.float32) for mask in masks]
    weights = split(jnp.concatenate([exact_nt(hot, layer[...]) for hot in hots], axis=0))
    mixers = [split(exact_nt(layer[...], hot)) for hot in hots]
    rate = jnp.concatenate([column(mask, rates[...]) for mask in masks], axis=0)
    for i, mask in enumerate(masks):
        gain_buf[i * padded : (i + 1) * padded] = jnp.broadcast_to(
            column(mask, gains[...]), (padded, LANES)
        )
    tile = 512 if length % 512 == 0 else LANES
    width = tile // LANES

    def generate(t, total):
        start = pl.multiple_of(t * tile, tile)
        spot = (start + lax.broadcasted_iota(jnp.int32, (nb, tile), 1)).astype(jnp.float32)
        band = (lax.broadcasted_iota(jnp.int32, (nb, tile), 0) + 1).astype(jnp.float32)
        turn = band * spot * (1.0 / length)
        sines, cosines = sincos((turn - jnp.floor(turn)) * (2.0 * math.pi))
        line = (start + lax.broadcasted_iota(jnp.int32, (8, tile), 1)).astype(jnp.float32) / length
        line = jnp.where(lax.broadcasted_iota(jnp.int32, (8, tile), 0) == 0, line, 0.0)
        embed = jnp.concatenate([cosines, sines, line], axis=0)
        before = jnp.dot(
            first_t[...], embed, precision=exact, preferred_element_type=jnp.float32
        )
        basis, slope = sincos(before)
        embed_buf[:, pl.ds(start, tile)] = embed
        basis_buf[:, pl.ds(start, tile)] = basis
        slope_buf[:, pl.ds(start, tile)] = slope
        raw = jnp.exp(-rate * line[:1]) * product(weights, split(basis))
        for j in range(width):
            piece = raw[:, j * LANES : (j + 1) * LANES]
            total = total + piece * piece
            row = pl.ds(pl.multiple_of((t * width + j) * 8, 8), 8)
            for h in range(2 * groups):
                raw_buf[h, row, :] = piece[h * 8 : (h + 1) * 8]
        return total

    total = lax.fori_loop(
        0, length // tile, generate, jnp.zeros((2 * padded, LANES), jnp.float32)
    )
    norm = jnp.sqrt(jnp.sum(total, axis=1, keepdims=True) + epsilon)
    inverse[...] = jnp.broadcast_to(1.0 / norm, inverse.shape)
    factor = 1.0 / math.sqrt(length)
    long = 1024 if length % 1024 == 0 else LANES

    def functionals(lags, base, mixer, projected):
        scale = inverse[pl.ds(base, padded), :][:, :1]
        weight = factor * scale
        if projected is not None:
            shift = -weight * scale * scale * jnp.sum(projected, axis=1, keepdims=True)
        speed = rate[base : base + padded]
        per = long // LANES
        run = lags.shape[2] // group
        first_chunk = base // 8

        def gather(t, fetch):
            lines = []
            for h in range(groups):
                lines.append(jnp.concatenate([fetch(h, t * per + j) for j in range(per)], axis=1))
            return jnp.concatenate(lines, axis=0)

        def lag_tile(h, r):
            b = lax.div(r, run)
            at = (r - b * run) * group
            if group == 8:
                at = pl.multiple_of(at, 8)
            value = lags[b, h, pl.ds(at, group), :]
            if group < 8:
                value = jnp.concatenate(
                    [value, jnp.zeros((8 - group, LANES), jnp.float32)], axis=0
                )
            return value

        def raw_tile(h, r):
            return raw_buf[first_chunk + h, pl.ds(pl.multiple_of(r * 8, 8), 8), :]

        def nt(left, right):
            one = lambda x, y: lax.dot_general(x, y, nt_dims, preferred_element_type=jnp.float32)
            return one(left[0], right[0]) + (one(left[1], right[0]) + one(left[0], right[1]))

        def step(t, sums_so_far):
            second_sum, first_sum, decay_sum = sums_so_far
            start = pl.multiple_of(t * long, long)
            embed = embed_buf[:, pl.ds(start, long)]
            line = embed[2 * nb : 2 * nb + 1]
            raw = gather(t, raw_tile)
            draw = gather(t, lag_tile) * weight
            if projected is not None:
                draw = draw + raw * shift
            moment = draw * raw * line
            for j in range(per):
                decay_sum = decay_sum - moment[:, j * LANES : (j + 1) * LANES]
            dmix = split(draw * jnp.exp(-speed * line))
            second_sum = second_sum + nt(dmix, split(basis_buf[:, pl.ds(start, long)]))
            dbasis = product(mixer, dmix) * slope_buf[:, pl.ds(start, long)]
            first_sum = first_sum + nt(split(embed), split(dbasis))
            return second_sum, first_sum, decay_sum

        order = basis_buf.shape[0]
        state = (
            jnp.zeros((padded, order), jnp.float32),
            jnp.zeros((embed_buf.shape[0], order), jnp.float32),
            jnp.zeros((padded, LANES), jnp.float32),
        )
        return lax.fori_loop(0, lags.shape[0] * run // per, step, state)

    second, third = (w2h[...], w2l[...]), (w3h[...], w3l[...])
    count = 2 if group % 2 == 0 else 1
    pairs = group // count
    rows = raw_buf.shape[1] // 8

    @pl.when(late)
    def _():
        own = me - half
        late_msg[...] = jnp.zeros(late_msg.shape, jnp.float32)
        first, last = (v1h[...], v1l[...]), (v4h[...], v4l[...])
        cos_t, sin_t = cv[...], sv[...]

        def chunk(g, carry):
            settle(late_cot.at[:, g], late_cot_got.at[g])
            settle(late_sig.at[:, g], late_sig_got.at[g])

            def step(p, carry):
                lanes = [p * count + j for j in range(count)]
                cots = [channel(late_cot, g, lane, group) for lane in lanes]
                sigs = [channel(late_sig, g, lane, group) for lane in lanes]
                raws = [
                    raw_buf[groups + g, pl.ds(lane, rows // 2, stride=8), :] for lane in lanes
                ]
                specs = forward(cots + sigs + raws, first, second, cos_t, sin_t)
                prods = [conjugate(specs[2 * count + j], specs[j]) for j in range(count)]
                prods += [conjugate(specs[count + j], specs[j]) for j in range(count)]
                values = backward(prods, third, last, cos_t, sin_t)
                for j, lane in enumerate(lanes):
                    at = pl.ds(padded + g * 8 + lane, 1)
                    gain = gain_buf[at, :]
                    put(late_cot, g, lane, group, values[j] * inverse[at, :] + gain * cots[j])
                    put(late_sig, g, lane, group, values[count + j])
                    at = pl.ds(g * 8 + lane, 1)
                    late_msg[0, at, :] = jnp.sum(
                        raws[j] * values[count + j], axis=0, keepdims=True
                    )
                    late_msg[1, at, :] = jnp.sum(cots[j] * sigs[j], axis=0, keepdims=True)
                return carry

            lax.fori_loop(0, pairs, step, 0)
            pltpu.make_async_copy(late_cot.at[own, g], in_out.at[own, g], ig_got).start()
            for k in range(1, half):
                to = lax.rem(own + k, half)
                send(late_cot.at[to, g], in_out.at[own, g], late_ig_sent, ig_got, to + half)
            return carry

        lax.fori_loop(0, groups, chunk, 0)
        second_sum, first_sum, decay_sum = functionals(late_sig, padded, mixers[1], None)
        late_msg[2] = decay_sum
        late_msg[3, :, : second_sum.shape[1]] = second_sum
        first_buf[...] = first_sum
        late_in[...] = jnp.zeros(late_in.shape, jnp.float32)
        send(late_msg, late_in, msg_sent, msg_got, own)

    first, last = (w1h[...], w1l[...]), (w4h[...], w4l[...])
    cos_t, sin_t = ct[...], st[...]

    def input_chunk(g, carry):
        settle(cot_buf.at[:, g], cot_got.at[g])

        def step(p, carry):
            lanes = [p * count + j for j in range(count)]
            cots = [channel(cot_buf, g, lane, group) for lane in lanes]
            raws = [raw_buf[g, pl.ds(lane, rows, stride=8), :] for lane in lanes]
            specs = forward(raws + cots, first, second, cos_t, sin_t)
            prods = [conjugate(specs[j], specs[count + j]) for j in range(count)]
            values = backward(prods, third, last, cos_t, sin_t)
            for j, lane in enumerate(lanes):
                gain = gain_buf[pl.ds(g * 8 + lane, 1), :]
                scale = inverse[pl.ds(g * 8 + lane, 1), :]
                put(ig_buf, g, lane, group, values[j] * scale + gain * cots[j])
            return carry

        lax.fori_loop(0, pairs, step, 0)
        pltpu.make_async_copy(ig_buf.at[me, g], in_out.at[me, g], ig_got).start()

        @pl.when(late)
        def _():
            for k in range(1, parts):
                to = lax.rem(me + k, parts)
                send(ig_buf.at[to, g], in_out.at[me, g], ig_sent, ig_got, to)

        @pl.when(jnp.logical_not(late))
        def _():
            for k in range(1, half):
                to = lax.rem(me + k, half)
                send(ig_buf.at[to, g], in_out.at[me, g], ig_sent, ig_got, to)

        return carry

    lax.fori_loop(0, groups, input_chunk, 0)

    def filter_chunk(g, carry):
        @pl.when(late)
        def _():
            settle(sig_buf.at[:, g], sig_got.at[g])

        @pl.when(jnp.logical_not(late))
        def _():
            settle(sig_buf.at[pl.ds(0, half), g], sig_got.at[g])

        def step(p, carry):
            lanes = [p * count + j for j in range(count)]
            cots = [channel(cot_buf, g, lane, group) for lane in lanes]
            sigs = [channel(sig_buf, g, lane, group) for lane in lanes]
            specs = forward(sigs + cots, first, second, cos_t, sin_t)
            prods = [conjugate(specs[j], specs[count + j]) for j in range(count)]
            values = backward(prods, third, last, cos_t, sin_t)
            for j, lane in enumerate(lanes):
                put(sig_buf, g, lane, group, values[j])
                at = pl.ds(g * 8 + lane, 1)
                raw = raw_buf[g, pl.ds(lane, rows, stride=8), :]
                skip[at, :] = jnp.sum(cots[j] * sigs[j], axis=0, keepdims=True)
                project[at, :] = jnp.sum(raw * values[j], axis=0, keepdims=True)
            return carry

        lax.fori_loop(0, pairs, step, 0)
        return carry

    lax.fori_loop(0, groups, filter_chunk, 0)

    @pl.when(jnp.logical_not(late))
    def _():
        settle(late_in, msg_got)

    second_sum, first_sum, decay_sum = functionals(
        sig_buf, 0, mixers[0], project[...] + late_in[0]
    )

    def row_of(value):
        value = jnp.sum(value, axis=1, keepdims=True)
        shape = (padded, LANES)
        same = lax.broadcasted_iota(jnp.int32, shape, 0) == lax.broadcasted_iota(jnp.int32, shape, 1)
        return jnp.sum(jnp.where(same, value, 0.0), axis=0, keepdims=True)

    order = basis_buf.shape[0]
    tall = embed_buf.shape[0]
    mine_buf[:padded, :order] = second_sum + late_in[3, :, :order]
    mine_buf[:tall, order:] = first_sum + first_buf[...]
    mine_buf[padded : padded + 1, :order] = row_of(decay_sum + late_in[2])[:, :order]
    mine_buf[padded + 1 : padded + 2, :order] = factor * row_of(skip[...] + late_in[1])[:, :order]

    copies = []
    for k in range(1, parts):
        copies.append(
            pltpu.make_async_remote_copy(
                src_ref=mine_buf,
                dst_ref=slots.at[k],
                send_sem=sends.at[k],
                recv_sem=arrivals.at[k],
                device_id=(lax.rem(me + k, parts), my_chan),
                device_id_type=MESH,
            )
        )
        copies[-1].start()
    slots[0] = mine_buf[...]
    for copy in copies:
        copy.wait_recv()
    acc = jnp.zeros(partial.shape, jnp.float32)
    blocks = []
    for b in range(parts):
        block = slots[lax.rem(me + parts - b, parts)]
        blocks.append(block[:padded])
        lines[b] = block[padded : padded + 8]
        acc = acc + block[:tall]
    partial[...] = acc
    for copy in copies:
        copy.wait_send()
    copies = []
    for k in range(1, chans):
        copies.append(
            pltpu.make_async_remote_copy(
                src_ref=partial,
                dst_ref=sums.at[k],
                send_sem=sends2.at[k],
                recv_sem=arrivals2.at[k],
                device_id=(me, lax.rem(my_chan + k, chans)),
                device_id_type=MESH,
            )
        )
        copies[-1].start()
    sums[0] = acc
    turned[...] = jnp.concatenate(blocks, axis=0).T[:order]
    for copy in copies:
        copy.wait_recv()
    acc = jnp.zeros_like(acc)
    for c in range(chans):
        acc = acc + sums[lax.rem(my_chan + chans - c, chans)]
    whole[...] = acc
    for copy in copies:
        copy.wait_send()

    settle(cot_in.at[pl.ds(0, parts - 1)], cot_sent)
    settle(in_out, ig_got)

    @pl.when(late)
    def _():
        settle(cot_in.at[pl.ds(0, 2 * (half - 1))], late_sent)
        settle(cot_in.at[pl.ds(0, half - 1)], late_ig_sent)
        settle(late_msg, msg_sent)
        settle(cot_in.at[pl.ds(0, half - 1)], sig_sent)
        settle(cot_in.at[pl.ds(0, parts - 1)], ig_sent)

    @pl.when(jnp.logical_not(late))
    def _():
        settle(cot_in.at[pl.ds(0, parts - 1)], sig_sent)
        settle(cot_in.at[pl.ds(0, half - 1)], ig_sent)


def run_block(sig, cot, first_t, layer, rates, gains, group, length, chans):
    parts, groups, run, _ = sig.shape
    half = parts // 2
    rows = length // LANES
    nb = (first_t.shape[1] - 8) // 2
    order, tall = first_t.shape
    padded = groups * 8
    high = max(-(-tall // 8) * 8, padded + 8)
    tabs = tables(rows, LANES)
    small = tables(rows // 2, LANES)
    small = (*small[:2], *small[6:])
    hbm = pl.BlockSpec(memory_space=pl.ANY)
    vmem = pl.BlockSpec(memory_space=pltpu.VMEM)
    dma = pltpu.SemaphoreType.DMA
    f32 = jnp.float32
    pieces = (first_t, layer, rates, gains, *tabs, *small)
    return pl.pallas_call(
        functools.partial(block_kernel, parts, chans, group, nb),
        in_specs=[hbm, hbm] + [vmem] * len(pieces),
        out_specs=[hbm, vmem, vmem, vmem],
        out_shape=[
            jax.ShapeDtypeStruct(sig.shape, f32),
            jax.ShapeDtypeStruct((order, parts * padded), f32),
            jax.ShapeDtypeStruct((parts, 8, LANES), f32),
            jax.ShapeDtypeStruct((tall, LANES), f32),
        ],
        scratch_shapes=[
            pltpu.VMEM(sig.shape, f32),
            pltpu.VMEM(sig.shape, f32),
            pltpu.VMEM(sig.shape, f32),
            pltpu.VMEM((half, groups, run, LANES), f32),
            pltpu.VMEM((half, groups, run, LANES), f32),
            pltpu.VMEM((2 * groups, rows * 8, LANES), f32),
            pltpu.VMEM((order, length), f32),
            pltpu.VMEM((order, length), f32),
            pltpu.VMEM((tall, length), f32),
            pltpu.VMEM((2 * padded, LANES), f32),
            pltpu.VMEM((2 * padded, LANES), f32),
            pltpu.VMEM((padded, LANES), f32),
            pltpu.VMEM((padded, LANES), f32),
            pltpu.VMEM((4, padded, LANES), f32),
            pltpu.VMEM((4, padded, LANES), f32),
            pltpu.VMEM((tall, order), f32),
            pltpu.VMEM((high, LANES), f32),
            pltpu.VMEM((parts, high, LANES), f32),
            pltpu.VMEM((tall, LANES), f32),
            pltpu.VMEM((chans, tall, LANES), f32),
            dma((groups,)),
            dma((groups,)),
            dma((groups,)),
            dma((groups,)),
            dma,
            dma,
            dma,
            dma,
            dma,
            dma,
            dma,
            dma,
            dma((parts,)),
            dma((parts,)),
            dma((chans,)),
            dma((chans,)),
        ],
        compiler_params=pltpu.CompilerParams(
            collective_id=1, has_side_effects=True, vmem_limit_bytes=67043328
        ),
        name="block",
    )(sig, cot, *pieces)


def local(signal, cotangent, first_layer, second_layer, decay_rate, skip_gain):
    parts = lax.axis_size("batch")
    width_dev, local_len = signal.shape
    bands, order = first_layer.shape
    length = local_len * parts
    narrow = width_dev // parts
    group = min(8, narrow)
    groups = narrow // group
    nb = bands // 2

    def tiles(x):
        x = x.reshape(parts, groups, group, local_len // LANES, LANES)
        return x.transpose(0, 1, 3, 2, 4).reshape(parts, groups, -1, LANES)

    first_t = jnp.concatenate([first_layer[1:], first_layer[:1]], axis=0)
    first_t = jnp.pad(first_t, ((0, 7), (0, 0))).T
    in_grad, turned, lines, total = run_block(
        tiles(signal),
        tiles(cotangent),
        first_t,
        second_layer,
        decay_rate.reshape(1, -1),
        skip_gain.reshape(1, -1),
        group,
        length,
        lax.axis_size("chan"),
    )
    input_grad = in_grad.reshape(parts, groups, local_len // LANES, group, LANES)
    input_grad = input_grad.transpose(0, 1, 3, 2, 4).reshape(width_dev, local_len)
    first_grad = total[: bands + 7, order:]
    first_grad = jnp.concatenate([first_grad[2 * nb : bands], first_grad[: 2 * nb]], axis=0)

    def kept(x):
        x = x.reshape(-1, parts * groups, 8)[:, :, :group]
        return x.reshape(-1, width_dev)

    second_grad = kept(turned) if group < 8 else turned
    rest = kept(lines[:, :2, : groups * 8].transpose(1, 0, 2))
    decay_grad, skip_grad = rest[0], rest[1]
    return (input_grad, first_grad, second_grad, decay_grad, skip_grad)


def solution(mesh):
    placed = (P("chan", "batch"), P("chan", "batch"), P(), P(None, "chan"), P("chan"), P("chan"))
    return jax.shard_map(
        local,
        mesh=mesh,
        in_specs=placed,
        out_specs=(P("chan", "batch"), P(), P(None, "chan"), P("chan"), P("chan")),
        check_vma=False,
    )
```
